32 devices in a mesh: hx: 4 (over y, x), hy: 4 (over z), tok: 2 (over core).
Axes of the slice: x: 2, y: 2, z: 4, core: 2. Of those that a mesh axis runs over, the one named last changes fastest.
Arguments:
- stream_in: bfloat16 [512, 4608], P('tok', ('hx', 'hy')), may hold values from -6 to 6
- before_gain: bfloat16 [4608], P(('hx', 'hy')), may hold values from 0.25 to 1.75
- after_gain: bfloat16 [4608], P(('hx', 'hy')), may hold values from 0.25 to 1.75
- feed_gain: bfloat16 [4608], P(('hx', 'hy')), may hold values from 0.25 to 1.75
- query_weight: bfloat16 [4608, 4096], P('tok', ('hx', 'hy')), may hold values from -1 to 1
- key_weight: bfloat16 [4608, 2048], P('tok', ('hx', 'hy')), may hold values from -64 to 64
- value_weight: bfloat16 [4608, 2048], P('tok', ('hx', 'hy')), may hold values from -0.09375 to 0.09375
- output_weight: bfloat16 [4096, 4608], P(('hx', 'hy'), 'tok'), may hold values from -0.09375 to 0.09375
- documents: int32 [512], P('tok'), may hold values from 0 to 7, never falling along the last dimension, each value on 1 to 128 neighbouring positions
Outputs:
- residual: bfloat16 [512, 4608], P('tok', ('hx', 'hy'))
- feed_input: bfloat16 [512, 4608], P('tok', ('hx', 'hy'))
The draws below stay inside these ranges and needn't reach their ends.
Inputs may be any that keep to these rules, and one draw needn't show every extreme that they name: `documents`: ids never fall along the tokens; a document holds at most 128 tokens and may run across a sequence's end.
All inputs are finite; a program needn't handle non-finite values.
Results may differ from the reference program's by a relative error of at most 0.014.
The reference program's roundings to bfloat16 on the way count: a program that leaves them out, or rounds other values in their place, can miss the bound.
Values may be sent and summed in bfloat16 or wider, within the bound.
A program may use at most 64 MiB of HBM per device.

```python
import math
import jax
import jax.numpy as jnp
import numpy as np
from jax import lax

D = 4608
QH = 32
KVH = 16
HEAD = 128
LENGTH = 256
TOKENS = 512
DOCS = 8
N_HX = 4
N_HY = 4


def query_base(key):
    return jax.random.truncated_normal(jax.random.fold_in(key, 11), -6.0, 6.0, (D, QH * HEAD), jnp.float32) * D ** (-0.5)


def draw_query_weight(key, part):
    return query_base(key).astype(jnp.bfloat16)


def draw_key_weight(key, part):
    independent = jax.random.truncated_normal(jax.random.fold_in(key, 23), -6.0, 6.0, (D, KVH * HEAD), jnp.float32) * D ** (-0.5)
    return independent.astype(jnp.bfloat16)


def steps_of(stream_key, shape, split, smallest, high):
    def one(position, shards_of):
        heights = jax.random.uniform(jax.random.fold_in(jax.random.fold_in(stream_key, 6), position), (shards_of,), jnp.float32, smallest / len(split), high / len(split))
        return jnp.repeat(jnp.exp(heights), shape[position] // shards_of).reshape((-1,) + (1,) * (len(shape) - position - 1))

    level = one(*split[0])
    for cut in split[1:]:
        level = level * one(*cut)
    return level


def split_up(amount, total, bound, lean):
    weights = [(1 << 20) // math.isqrt(standing ** lean) + 1 for standing in range(2, amount + 1)]
    surplus, counts = total - bound - (amount - 1), [1] * (amount - 1)
    while surplus > 0:
        candidates = [i for i in range(amount - 1) if counts[i] < bound]
        whole, left = sum([weights[i] for i in candidates]), surplus
        for i in candidates:
            more = min(bound - counts[i], max(1, left * weights[i] // whole), surplus)
            counts[i] = counts[i] + more
            surplus = surplus - more
    return np.array([bound] + counts)


def uneven_parts(rng, amount, total, limit, skew):
    if amount == 2:
        one = jax.random.randint(rng, (), max(1, total - limit), min(limit, total - 1) + 1)
        return jnp.stack([one, total - one])
    lengths = jnp.asarray(split_up(amount, total, limit, skew), jnp.int32)
    pairs = (amount - 1) // 2
    donor, receiver = lengths[1:1 + 2 * pairs:2], lengths[2:2 + 2 * pairs:2]
    margin = jnp.minimum(donor - 1, limit - receiver)
    passed = jax.random.randint(jax.random.fold_in(rng, 1), (pairs,), 0, 1 << 20) % (margin + 1)
    lengths = lengths.at[1:1 + 2 * pairs:2].set(donor - passed).at[2:2 + 2 * pairs:2].set(receiver + passed)
    return lengths[jax.random.permutation(jax.random.fold_in(rng, 2), amount)]


def scatter_about(stream_key, shape, width, reach, cuts=(), kind=jnp.bfloat16):
    values = jax.random.normal(stream_key, shape, jnp.float32) * width
    if len(cuts) > 0:
        values = steps_of(stream_key, shape, cuts, -0.22, 0.18) * values
    return jnp.clip(values, min=-reach, max=reach).astype(kind)


def setup_inputs(seed: int = 0) -> dict:
    seeds = jax.random.split(jax.random.key(seed), 10)
    stream_in = scatter_about(seeds[0], (TOKENS, D), 1.0, 6.0, ((0, 2), (1, 16)))
    before_gain = jnp.clip(1.0 + 0.15 * jax.random.normal(seeds[1], (D,), jnp.float32), 0.25, 1.75).astype(jnp.bfloat16)
    after_gain = jnp.clip(1.0 + 0.15 * jax.random.normal(seeds[2], (D,), jnp.float32), 0.25, 1.75).astype(jnp.bfloat16)
    feed_gain = jnp.clip(1.0 + 0.15 * jax.random.normal(seeds[3], (D,), jnp.float32), 0.25, 1.75).astype(jnp.bfloat16)
    query_weight = draw_query_weight(jax.random.fold_in(seeds[9], 71), 0)
    key_weight = draw_key_weight(jax.random.fold_in(seeds[9], 71), 0)
    value_weight = scatter_about(seeds[6], (D, KVH * HEAD), D ** -0.5, 0.09375, ((0, 2), (1, 16)))
    output_weight = scatter_about(seeds[7], (QH * HEAD, D), (QH * HEAD) ** -0.5, 0.09375, ((0, 16), (1, 2)))
    documents = jnp.searchsorted(jnp.cumsum(uneven_parts(seeds[8], DOCS, TOKENS, LENGTH // 2, 0)), jnp.arange(TOKENS), side="right").astype(jnp.int32)
    return {"stream_in": stream_in, "before_gain": before_gain, "after_gain": after_gain, "feed_gain": feed_gain, "query_weight": query_weight, "key_weight": key_weight, "value_weight": value_weight, "output_weight": output_weight, "documents": documents}


epsilon = 1e-06
neg_big = -1e+30

def rotate(values, positions):
    half_width = values.shape[-1] // 2
    frequency = 10000.0 ** (-jnp.arange(half_width, dtype=jnp.float32) / half_width)
    angles = positions.astype(jnp.float32)[:, None] * frequency[None, :]
    cosine_table = jnp.cos(angles)[:, None, :]
    sine_table = jnp.sin(angles)[:, None, :]
    leading = values[..., :half_width]
    trailing = values[..., half_width:]
    return jnp.concatenate([leading * cosine_table - trailing * sine_table, trailing * cosine_table + leading * sine_table], axis=-1)

def norm_rows(values, gain):
    squares = lax.optimization_barrier(jnp.sum(values * values, axis=-1, keepdims=True))
    return values * lax.rsqrt(squares / D + epsilon) * gain.astype(jnp.float32)[None, :]

def reference(stream_in, before_gain, after_gain, feed_gain, query_weight, key_weight, value_weight, output_weight, documents):
    wide = stream_in.astype(jnp.float32)
    normed = norm_rows(wide, before_gain).astype(jnp.bfloat16)
    positions = (jnp.arange(TOKENS) % LENGTH).astype(jnp.int32)
    query_sum = jnp.dot(normed, query_weight, preferred_element_type=jnp.float32)
    key_sum = jnp.dot(normed, key_weight, preferred_element_type=jnp.float32)
    value_sum = jnp.dot(normed, value_weight, preferred_element_type=jnp.float32)
    queries = (rotate(query_sum.reshape(TOKENS, QH, HEAD), positions) * (D / QH) ** (-0.5)).astype(jnp.bfloat16)
    keys = rotate(key_sum.reshape(TOKENS, KVH, HEAD), positions).astype(jnp.bfloat16)
    values = value_sum.reshape(TOKENS, KVH, HEAD).astype(jnp.bfloat16)
    ratio = QH // KVH
    count_seq = TOKENS // LENGTH
    query_seq = queries.reshape(count_seq, LENGTH, KVH, ratio, HEAD)
    key_seq = keys.reshape(count_seq, LENGTH, KVH, HEAD)
    value_seq = values.reshape(count_seq, LENGTH, KVH, HEAD)
    doc_seq = documents.reshape(count_seq, LENGTH)

    def one_sequence(items):
        query_part, key_part, value_part, doc_part = items
        scores = jnp.einsum('tkrh,skh->tkrs', query_part.astype(jnp.float32), key_part.astype(jnp.float32))
        index = jnp.arange(LENGTH)
        allowed = (index[None, :] <= index[:, None]) & (doc_part[None, :] == doc_part[:, None])
        mask = allowed[:, None, None, :]
        best = lax.optimization_barrier(jnp.max(jnp.where(mask, scores, neg_big), axis=-1, keepdims=True))
        weights = jnp.where(mask, jnp.exp(scores - best), 0.0)
        total = lax.optimization_barrier(jnp.sum(weights, axis=-1))
        weights_low = lax.optimization_barrier(weights.astype(jnp.bfloat16)).astype(jnp.float32)
        summed = jnp.einsum('tkrs,skh->tkrh', weights_low, value_part.astype(jnp.float32))
        return (summed / total[..., None]).astype(jnp.bfloat16)
    attended = lax.map(one_sequence, (query_seq, key_seq, value_seq, doc_seq)).reshape(TOKENS, QH * HEAD)
    groups = N_HX * N_HY
    span = QH * HEAD // groups
    mixed = jnp.zeros((TOKENS, D), jnp.float32)
    for group in range(groups):
        term = jnp.dot(attended[:, group * span:(group + 1) * span], output_weight[group * span:(group + 1) * span, :], preferred_element_type=jnp.float32)
        mixed = mixed + lax.optimization_barrier(term.astype(jnp.bfloat16)).astype(jnp.float32)
    residual = (wide + norm_rows(mixed, after_gain)).astype(jnp.bfloat16)
    feed_input = norm_rows(residual.astype(jnp.float32), feed_gain).astype(jnp.bfloat16)
    return (residual, feed_input)
```

```python
import functools

import jax
import jax.numpy as jnp
import numpy as np
from jax import lax
from jax.experimental import pallas as pl
from jax.experimental.pallas import tpu as pltpu
from jax.sharding import PartitionSpec as P

D = 4608
QH = 32
HEAD = 128
LENGTH = 256
LANES = 128

epsilon = 1e-06
neg_big = -1e30
MESH = pl.DeviceIdType.MESH
F32 = jnp.float32
BF16 = jnp.bfloat16


GATHER = {
    "A": ("", "z1", "z2", "z3", "x", "x", "x", "z1", "y", "y", "y", "z1", "x", "z1", "x", "x"),
    "B": ("", "z1", "z2", "z3", "x", "z1", "z1", "x", "y", "y", "y", "y", "y", "y", "x", "x"),
}
REDUCE = {
    "A": ("", "z1", "z2", "z3", "z1", "x", "x", "z1", "y", "y", "y", "y", "x", "y", "x", "z1"),
    "B": ("", "z1", "z2", "z3", "z1", "x", "x", "x", "y", "y", "y", "y", "x", "z1", "y", "x"),
}
ORDER = (
    "hz", "s10B", "s02A", "s20B", "s20A", "s01A", "s03B", "hw", "hm", "s10A",
    "s30A", "s22A", "s11B", "s02B", "s01B", "s12A", "head", "p10A", "s21A", "s11A",
    "s23B", "s23A", "p00B", "s31A", "p20A", "s13B", "s32A", "p02A", "p11B", "s03A",
    "s31B", "p11A", "s22B", "p21A", "p10B", "s33B", "s21B", "p22A", "p12A", "p03B",
    "turn", "p13B", "s33A", "p01B", "s30B", "p00A", "p02B", "s13A", "p30A", "p32A",
    "p01A", "p23B", "s12B", "s32B", "p31A", "p33B", "p23A", "p20B", "p22B", "p21B",
    "p31B", "p33A", "p03A", "p13A", "aA", "t33A", "u33A", "p30B", "t23A", "u23A",
    "p32B", "p12B", "aB", "t32B", "t10A", "u10A", "u32B", "t21B", "t13A", "t13B",
    "t12A", "u13B", "t32A", "t22B", "t22A", "t33B", "t23B", "t31A", "t03A", "t01A",
    "t31B", "t21A", "t10B", "t03B", "u31A", "u10B", "t12B", "t00A", "t30A", "t01B",
    "u33B", "u22B", "u21B", "t02A", "t00B", "t02B", "u13A", "u12B", "u31B", "u03A",
    "u32A", "u21A", "t11A", "u23B", "u11A", "u02B", "u12A", "u30A", "t20A", "t30B",
    "t20B", "t11B", "u22A", "u11B", "u01A", "u03B", "u30B", "u02A", "u20A", "u01B",
    "u20B", "finA", "finB",
)


def flip(index, mask):
    low = (index % 2 + mask % 2) % 2
    high = (index // 2 + mask // 2) % 2
    return low + 2 * high


def rope_tables():
    half = HEAD // 2
    frequency = (10000.0 ** (-np.arange(half, dtype=np.float32) / half)).astype(np.float32)
    angles = frequency[:, None] * np.arange(LENGTH, dtype=np.float32)[None, :]
    return np.stack([np.cos(angles), np.sin(angles)]).astype(np.float32)


def tall_row(row):
    return jnp.broadcast_to(row, (8, row.shape[1]))


def tall(block):
    return jnp.concatenate([block] * (LANES // block.shape[0]), axis=0).T


def parent(block, link):
    i, j = block
    if link == "x":
        return i ^ 1, j
    if link == "y":
        return i ^ 2, j
    return i, j ^ int(link[1])


def kernel(
    paired,
    stream, docs, before, after_in, feed_in, tables, wq, wk, wv, wo,
    outs,
    slots, docs_v, before_v, after_v, feed_v, branch_v, tables_v, weights, out_weight, out_t, acc, keys, values, attended,
    terms, shares, head, head_z, head_mid, head_plane, stats, stats_in, stats_mid, stats_zin,
    local_sem, weight_send, weight_recv, gather_send, gather_recv, reduce_send, reduce_recv,
    head_send, head_recv, stat_send, stat_recv,
):
    width, rows = stream.shape
    rest = width - rows
    span = rows // 2
    a, b, c = lax.axis_index("hx"), lax.axis_index("hy"), lax.axis_index("tok")
    along_x, along_y, across = flip(a, 1), flip(a, 2), flip(a, 3)
    plane = (None, along_x, along_y, across)
    z_peers = [None] + [flip(b, j) for j in (1, 2, 3)]
    peers = {"x": {"hx": along_x}, "y": {"hx": along_y}}
    for j in (1, 2, 3):
        peers["z" + str(j)] = {"hy": z_peers[j]}

    def offset_of(i, j):
        return pl.multiple_of((flip(a, i) * 4 + flip(b, j)) * width, 16)

    locals_ = [
        pltpu.make_async_copy(stream.at[:, pl.ds(0, span)], slots.at[0, 0], local_sem.at[0]),
        pltpu.make_async_copy(stream.at[:, pl.ds(span, span)], slots.at[1, 0], local_sem.at[9]),
        pltpu.make_async_copy(before, before_v, local_sem.at[1]),
        pltpu.make_async_copy(tables, tables_v, local_sem.at[2]),
        pltpu.make_async_copy(docs, docs_v, local_sem.at[7]),
        pltpu.make_async_copy(after_in, after_v, local_sem.at[8]),
        pltpu.make_async_copy(feed_in, feed_v, local_sem.at[10]),
    ]
    for copy in locals_:
        copy.start()
    wrows, qcols, kcols = wq.shape[0], wq.shape[1], wk.shape[1]
    shard = c if paired else 0
    start = pl.multiple_of(shard * wrows, 16)
    targets = [
        (wq, weights.at[pl.ds(start, wrows), pl.ds(0, qcols)]),
        (wk, weights.at[pl.ds(start, wrows), pl.ds(qcols, kcols)]),
        (wv, weights.at[pl.ds(start, wrows), pl.ds(qcols + kcols, kcols)]),
        (wo, out_weight.at[shard]),
    ]
    weight_local = [
        pltpu.make_async_copy(src, dst, local_sem.at[3 + k]) for k, (src, dst) in enumerate(targets)
    ]

    barrier = pltpu.get_barrier_semaphore()
    greet = [{"hx": along_x}, {"hx": along_y}, {"hx": across}]
    greet += [{"hy": z_peers[j]} for j in (1, 2, 3)]
    if paired:
        greet.append({"tok": 1 - c})
    for peer in greet:
        pl.semaphore_signal(barrier, inc=1, device_id=peer, device_id_type=MESH)
    for copy in weight_local:
        copy.start()

    row8 = lax.broadcasted_iota(jnp.int32, (8, rows), 0)
    for copy in locals_[:3]:
        copy.wait()
    own = jnp.concatenate([slots[0, 0], slots[1, 0]], axis=1).astype(F32)

    def padded(vector):
        wide_vector = vector.astype(F32).reshape(1, width)
        return jnp.concatenate([wide_vector, jnp.zeros((1, rows + LANES - width), F32)], axis=1)

    before_row = padded(before_v[...])
    padded_tail = jnp.concatenate([before_row[:, rows:], jnp.zeros((1, rows - LANES), F32)], axis=1)
    head[...] = jnp.where(
        row8 == 0,
        jnp.sum(own * own, axis=0, keepdims=True),
        jnp.where(row8 == 1, before_row[:, :rows], jnp.where(row8 == 2, padded_tail, 0.0)),
    )
    pl.semaphore_wait(barrier, len(greet))

    def remote(src, dst, send, recv, peer):
        return pltpu.make_async_remote_copy(
            src_ref=src, dst_ref=dst, send_sem=send, recv_sem=recv, device_id=peer, device_id_type=MESH
        )

    def head_to_z(j):
        return remote(head, head_z.at[j - 1], head_send.at[j - 1], head_recv.at[j - 1], {"hy": z_peers[j]})

    def head_to_plane(i):
        return remote(head_mid, head_plane.at[i - 1], head_send.at[2 + i], head_recv.at[2 + i], {"hx": plane[i]})

    def gather(block, h):
        link = GATHER["AB"[h]][4 * block[0] + block[1]]
        origin = parent(block, link)
        k = 4 * block[0] + block[1]
        return remote(
            slots.at[h, 4 * origin[0] + origin[1]], slots.at[h, k], gather_send.at[h, k], gather_recv.at[h, k], peers[link]
        )

    def share(block, h):
        k = 4 * block[0] + block[1]
        link = REDUCE["AB"[h]][k]
        return remote(terms.at[h, k], shares.at[h, k], reduce_send.at[h, k], reduce_recv.at[h, k], peers[link])

    blocks = [(i, j) for i in range(4) for j in range(4)]
    children = {(h, block): [] for h in range(2) for block in blocks}
    for h in range(2):
        for block in blocks[1:]:
            link = REDUCE["AB"[h]][4 * block[0] + block[1]]
            children[h, parent(block, link)].append(block)

    weight_remote = []
    if paired:
        weight_remote = [
            remote(src, dst, weight_send.at[k], weight_recv.at[k], {"tok": 1 - c})
            for k, (src, dst) in enumerate(targets)
        ]
    state = {}
    arrived = set()

    def await_gather(block, h):
        if block != (0, 0) and ("g", block, h) not in arrived:
            arrived.add(("g", block, h))
            gather(block, h).wait_recv()

    def send_heads():
        for j in (3, 2, 1):
            head_to_z(j).start()

    def send_weights():
        for copy in weight_remote:
            copy.start()

    def relay_heads():
        for j in (1, 2, 3):
            head_to_z(j).wait_recv()
        mains = [head[...]] + [head_z[j] for j in range(3)]
        total = mains[0] + mains[1] + mains[2] + mains[3]
        tails = jnp.zeros((1, rows), F32)
        for j in range(4):
            part = mains[j][2:3, :LANES]
            if j:
                part = pltpu.roll(tall_row(part), j * rest, 1)[0:1]
            tails = tails + jnp.concatenate([part, jnp.zeros((1, rows - LANES), F32)], axis=1)
        mid = jnp.where(row8 == 0, total[0:1], 0.0)
        for j in range(4):
            mid = jnp.where(row8 == 1 + j, mains[j][1:2], mid)
        head_mid[...] = jnp.where(row8 == 5, tails, mid)
        for i in (3, 1, 2):
            head_to_plane(i).start()

    def use_heads():
        for i in (1, 2, 3):
            head_to_plane(i).wait_recv()
        groups = [head_mid[...]] + [head_plane[i] for i in range(3)]
        state["first_sq"] = groups[0][0:1] + groups[1][0:1] + groups[2][0:1] + groups[3][0:1]
        state["first_scale"] = lax.rsqrt(state["first_sq"] / D + epsilon)
        state["gain_columns"] = tall(jnp.concatenate(groups, axis=0))
        for copy in weight_local[:3]:
            copy.wait()
        for copy in weight_remote[:3]:
            copy.wait_recv()

    def project(block, h):
        await_gather(block, h)
        i, j = block
        gain_columns = state["gain_columns"]
        gain = jnp.concatenate(
            [gain_columns[:, 8 * i + 1 + j:8 * i + 2 + j], gain_columns[j * rest:(j + 1) * rest, 8 * i + 5:8 * i + 6]],
            axis=0,
        )
        scale = state["first_scale"][:, h * span:(h + 1) * span]
        normed = (slots[h, 4 * i + j].astype(F32) * scale * gain).astype(BF16)
        part = lax.dot_general(
            weights[pl.ds(offset_of(i, j), width), :], normed, (((0,), (0,)), ((), ())), preferred_element_type=F32
        )
        if ("p", h) not in arrived:
            arrived.add(("p", h))
            acc[h] = part
        else:
            acc[h] += part

    shards, depth, columns = out_weight.shape

    def turn():
        weight_local[3].wait()
        for copy in weight_remote[3:]:
            copy.wait_recv()
        for copy in locals_[3:]:
            copy.wait()
        step = 3 * LANES
        for k in range(D // step):
            s, at = (k * step) // columns, (k * step) % columns
            out_t[k * step:(k + 1) * step, :] = out_weight[s, :, at:at + step].T
        doc_row = docs_v[...].astype(F32)
        after_row = padded(after_v[...])
        state["doc_row"] = doc_row
        state["doc_col"] = tall(jnp.broadcast_to(doc_row, (8, rows)))[:, 0:1]
        feed_row = padded(feed_v[...])
        state["feed"] = tall(jnp.broadcast_to(feed_row, (8, rows + LANES)))[:width, 0:1]
        state["after"] = tall(jnp.broadcast_to(after_row, (8, rows + LANES)))[:width, 0:1]

    query_heads, key_heads = qcols // HEAD, kcols // HEAD
    ratio = query_heads // key_heads

    def attend(h):
        lanes = slice(h * span, (h + 1) * span)
        seen = (h + 1) * span
        cosine, sine = tables_v[0, :, lanes], tables_v[1, :, lanes]

        def rope(x):
            upper, lower = x[:HEAD // 2], x[HEAD // 2:]
            return jnp.concatenate([upper * cosine - lower * sine, lower * cosine + upper * sine], axis=0)

        for kv in range(key_heads):
            keys[kv, :, lanes] = rope(acc[h, qcols + kv * HEAD:qcols + (kv + 1) * HEAD]).astype(BF16)
            values[kv, :, lanes] = acc[h, qcols + kcols + kv * HEAD:qcols + kcols + (kv + 1) * HEAD].astype(BF16)
        s_index = lax.broadcasted_iota(jnp.int32, (seen, span), 0)
        t_index = lax.broadcasted_iota(jnp.int32, (seen, span), 1) + h * span
        allowed = (s_index <= t_index) & (state["doc_row"][:, lanes] == state["doc_col"][:seen])
        for q in range(query_heads):
            query = (rope(acc[h, q * HEAD:(q + 1) * HEAD]) * (D / QH) ** (-0.5)).astype(BF16)
            key, value = keys[q // ratio, :, :seen], values[q // ratio, :, :seen]
            scores = lax.dot_general(key, query, (((0,), (0,)), ((), ())), preferred_element_type=F32)
            best = jnp.max(jnp.where(allowed, scores, neg_big), axis=0, keepdims=True)
            soft = jnp.where(allowed, jnp.exp(scores - best), 0.0)
            mass = jnp.sum(soft, axis=0, keepdims=True)
            blended = jnp.dot(value, soft.astype(BF16), preferred_element_type=F32)
            attended[h, q * HEAD:(q + 1) * HEAD, :] = (blended / mass).astype(BF16)

    def term(block, h):
        at = offset_of(*block)
        terms[h, 4 * block[0] + block[1]] = jnp.dot(
            out_t[pl.ds(at, width), :], attended[h], preferred_element_type=F32
        ).astype(BF16)

    def collect(block, h):
        for child in children[h, block]:
            share(child, h).wait_recv()
        total = terms[h, 4 * block[0] + block[1]].astype(F32)
        for child in children[h, block]:
            total = total + shares[h, 4 * child[0] + child[1]].astype(F32)
        return total

    def pass_on(block, h):
        if children[h, block]:
            terms[h, 4 * block[0] + block[1]] = collect(block, h).astype(BF16)
        share(block, h).start()

    def finish(h):
        mixed = collect((0, 0), h)
        lanes = slice(h * span, (h + 1) * span)
        wide = slots[h, 0].astype(F32)
        branch = mixed * state["after"]
        narrow = row8[:, :span]
        stats[:, lanes] = jnp.where(
            narrow == 0,
            jnp.sum(mixed * mixed, axis=0, keepdims=True),
            jnp.where(
                narrow == 1,
                jnp.sum(wide * branch, axis=0, keepdims=True),
                jnp.sum(branch * branch, axis=0, keepdims=True),
            ),
        )
        branch_v[:, lanes] = branch

    for task in ORDER:
        if task == "hz":
            send_heads()
        elif task == "hw":
            send_weights()
        elif task == "hm":
            relay_heads()
        elif task == "head":
            use_heads()
        elif task == "turn":
            turn()
        elif task[:3] == "fin":
            finish("AB".index(task[3]))
        elif task[0] == "a":
            attend("AB".index(task[1]))
        else:
            block, h = (int(task[1]), int(task[2])), "AB".index(task[3])
            if task[0] == "s":
                copy = gather(block, h)
                await_gather(parent(block, GATHER["AB"[h]][4 * block[0] + block[1]]), h)
                copy.start()
            elif task[0] == "p":
                project(block, h)
            elif task[0] == "t":
                term(block, h)
            elif task[0] == "u":
                pass_on(block, h)

    def stat_plane(i):
        return remote(stats, stats_in.at[i - 1], stat_send.at[i - 1], stat_recv.at[i - 1], {"hx": plane[i]})

    def stat_z(j):
        return remote(stats_mid, stats_zin.at[j - 1], stat_send.at[2 + j], stat_recv.at[2 + j], {"hy": z_peers[j]})

    for i in (3, 2, 1):
        stat_plane(i).start()
    for i in (1, 2, 3):
        stat_plane(i).wait_recv()
    stats_mid[...] = stats[...] + stats_in[0] + stats_in[1] + stats_in[2]
    for j in (3, 2, 1):
        stat_z(j).start()
    for h in range(2):
        for block in blocks[1:]:
            gather(block, h).wait_send()
            share(block, h).wait_send()
    for j in (1, 2, 3):
        head_to_z(j).wait_send()
        head_to_plane(j).wait_send()
        stat_plane(j).wait_send()
    for copy in weight_remote:
        copy.wait_send()
    for j in (1, 2, 3):
        stat_z(j).wait_recv()
    summed = stats_mid[...] + stats_zin[0] + stats_zin[1] + stats_zin[2]
    after_scale = lax.rsqrt(summed[0:1] / D + epsilon)
    feed_sq = state["first_sq"] + 2.0 * after_scale * summed[1:2] + after_scale * after_scale * summed[2:3]
    feed_scale = lax.rsqrt(feed_sq / D + epsilon)
    for h in range(2):
        lanes = slice(h * span, (h + 1) * span)
        residual = (slots[h, 0].astype(F32) + branch_v[:, lanes] * after_scale[:, lanes]).astype(BF16)
        outs[0, :, lanes] = residual
        outs[1, :, lanes] = (residual.astype(F32) * feed_scale[:, lanes] * state["feed"]).astype(BF16)
    for j in (1, 2, 3):
        stat_z(j).wait_send()


def per_device(paired, stream_in, before_gain, after_gain, feed_gain, query_weight, key_weight, value_weight, output_weight, documents):
    rows, width = stream_in.shape
    if not paired:
        query_weight, key_weight, value_weight = (
            lax.all_gather(piece, "tok", axis=0, tiled=True) for piece in (query_weight, key_weight, value_weight)
        )
        output_weight = lax.all_gather(output_weight, "tok", axis=1, tiled=True)
    tables = jnp.asarray(rope_tables())
    qcols, kcols = query_weight.shape[1], key_weight.shape[1]
    shards = 2 if paired else 1
    depth = output_weight.shape[0]
    any_spec = pl.BlockSpec(memory_space=pl.ANY)
    vmem = pl.BlockSpec(memory_space=pltpu.VMEM)
    dma = pltpu.SemaphoreType.DMA
    block, piece = (width, rows), (width, rows // 2)
    both = pl.pallas_call(
        functools.partial(kernel, paired),
        out_shape=jax.ShapeDtypeStruct((2,) + block, BF16),
        in_specs=[any_spec] * 10,
        out_specs=vmem,
        scratch_shapes=[
            pltpu.VMEM((2, 16) + piece, BF16),
            pltpu.VMEM((1, rows), jnp.int32),
            pltpu.VMEM((width,), BF16),
            pltpu.VMEM((width,), BF16),
            pltpu.VMEM((width,), BF16),
            pltpu.VMEM(block, F32),
            pltpu.VMEM((2, HEAD // 2, LENGTH), F32),
            pltpu.VMEM((D, qcols + 2 * kcols), BF16),
            pltpu.VMEM((shards, depth, output_weight.shape[1]), BF16),
            pltpu.VMEM((D, depth), BF16),
            pltpu.VMEM((2, qcols + 2 * kcols, rows // 2), F32),
            pltpu.VMEM((kcols // HEAD, HEAD, rows), BF16),
            pltpu.VMEM((kcols // HEAD, HEAD, rows), BF16),
            pltpu.VMEM((2, qcols, rows // 2), BF16),
            pltpu.VMEM((2, 16) + piece, BF16),
            pltpu.VMEM((2, 16) + piece, BF16),
        ]
        + [pltpu.VMEM((8, rows), F32), pltpu.VMEM((3, 8, rows), F32)] * 4
        + [
            dma((11,)),
            dma((4,)),
            dma((4,)),
            dma((2, 16)),
            dma((2, 16)),
            dma((2, 16)),
            dma((2, 16)),
            dma((6,)),
            dma((6,)),
            dma((6,)),
            dma((6,)),
        ],
        compiler_params=pltpu.CompilerParams(
            collective_id=0, has_side_effects=True, vmem_limit_bytes=56 * 1024 * 1024
        ),
    )(
        stream_in.T,
        documents.reshape(1, rows),
        before_gain,
        after_gain,
        feed_gain,
        tables,
        query_weight,
        key_weight,
        value_weight,
        output_weight,
    )
    return both[0].T, both[1].T


def solution(mesh):
    both = ("hx", "hy")
    in_specs = (
        P("tok", both),
        P(both),
        P(both),
        P(both),
        P("tok", both),
        P("tok", both),
        P("tok", both),
        P(both, "tok"),
        P("tok"),
    )
    out_specs = (P("tok", both), P("tok", both))
    paired = mesh.shape["tok"] == 2
    return jax.shard_map(
        functools.partial(per_device, paired), mesh=mesh, in_specs=in_specs, out_specs=out_specs, check_vma=False
    )
```

```python
import functools

import jax
import jax.numpy as jnp
import numpy as np
from jax import lax
from jax.experimental import pallas as pl
from jax.experimental.pallas import tpu as pltpu
from jax.sharding import PartitionSpec as P

D = 4608
QH = 32
HEAD = 128
LENGTH = 256
LANES = 128

epsilon = 1e-06
neg_big = -1e30
MESH = pl.DeviceIdType.MESH
F32 = jnp.float32
BF16 = jnp.bfloat16


GATHER = {
    "A": ("", "z1", "z1", "z3", "x", "x", "z1", "x", "y", "y", "y", "y", "d", "z1", "z1", "d"),
    "B": ("", "z1", "z2", "z1", "x", "x", "x", "z1", "y", "y", "y", "y", "x", "z1", "x", "d"),
}
REDUCE = {
    "A": ("", "z1", "z2", "z3", "x", "x", "x", "z1", "y", "y", "y", "y", "x", "z1", "y", "x"),
    "B": ("", "z1", "z2", "z1", "x", "x", "x", "x", "y", "y", "y", "z1", "d", "z1", "y", "x"),
}
ORDER = (
    "s10A", "s20A", "s10B", "s30A", "hz", "s01A", "s20B", "s03A", "hw", "hm", "s01B", "s02B",
    "s11A", "s21A", "s33A", "s02A", "s13A", "s30B", "head", "n21A", "n10B", "s31A", "n20B", "s23A",
    "turn", "s03B", "s22B", "s12B", "s22A", "s11B", "s12A", "n03A", "n02B", "n30A", "n11A", "n00A",
    "n02A", "n23A", "s21B", "n01A", "m0A", "s32A", "n33A", "n31A", "n03B", "s23B", "s32B", "s31B",
    "n01B", "n20A", "n30B", "n00B", "n22B", "m0B", "n10A", "n12B", "s13B", "n13A", "n22A", "s33B",
    "n12A", "m2A", "m1A", "n11B", "n32A", "m3A", "aA", "n32B", "t1A", "t3A", "u31A", "u33A",
    "n21B", "u32A", "u11A", "u13A", "n23B", "t2A", "m2B", "n31B", "u21A", "n13B", "m1B", "n33B",
    "m3B", "aB", "t3B", "u33B", "u31B", "u32B", "t1B", "u13B", "u11B", "t0B", "t0A", "u23A",
    "t2B", "u22A", "u01A", "u12A", "u30A", "u21B", "u23B", "u12B", "u20B", "u03B", "u03A", "u10B",
    "u22B", "u02A", "u01B", "u10A", "u20A", "u30B", "u02B", "finA", "finB",
)


def flip(index, mask):
    low = (index % 2 + mask % 2) % 2
    high = (index // 2 + mask // 2) % 2
    return low + 2 * high


def rope_tables():
    half = HEAD // 2
    frequency = (10000.0 ** (-np.arange(half, dtype=np.float32) / half)).astype(np.float32)
    angles = frequency[:, None] * np.arange(LENGTH, dtype=np.float32)[None, :]
    return np.stack([np.cos(angles), np.sin(angles)]).astype(np.float32)


def tall_row(row):
    return jnp.broadcast_to(row, (8, row.shape[1]))


def tall(block):
    return jnp.concatenate([block] * (LANES // block.shape[0]), axis=0).T


def parent(block, link):
    i, j = block
    if link == "x":
        return i ^ 1, j
    if link == "y":
        return i ^ 2, j
    if link == "d":
        return i ^ 3, j
    return i, j ^ int(link[1])


def kernel(
    paired,
    stream, docs, before, after_in, feed_in, tables, wq, wk, wv, wo,
    outs,
    slots, docs_v, before_v, after_v, feed_v, branch_v, tables_v, weights, out_weight, out_t, acc, keys, values, attended,
    normed, terms, shares, head, head_z, head_mid, head_plane, stats, stats_in, stats_mid, stats_zin,
    local_sem, weight_send, weight_recv, gather_send, gather_recv, reduce_send, reduce_recv,
    head_send, head_recv, stat_send, stat_recv,
):
    width, rows = stream.shape
    rest = width - rows
    span = rows // 2
    a, b, c = lax.axis_index("hx"), lax.axis_index("hy"), lax.axis_index("tok")
    along_x, along_y, across = flip(a, 1), flip(a, 2), flip(a, 3)
    plane = (None, along_x, along_y, across)
    z_peers = [None] + [flip(b, j) for j in (1, 2, 3)]
    peers = {"x": {"hx": along_x}, "y": {"hx": along_y}, "d": {"hx": across}}
    for j in (1, 2, 3):
        peers["z" + str(j)] = {"hy": z_peers[j]}

    def group(i):
        return pl.multiple_of(flip(a, i) * (4 * width), 16)

    def within(j):
        return pl.multiple_of(flip(b, j) * width, 16)

    locals_ = [
        pltpu.make_async_copy(stream.at[:, pl.ds(0, span)], slots.at[0, 0], local_sem.at[0]),
        pltpu.make_async_copy(stream.at[:, pl.ds(span, span)], slots.at[1, 0], local_sem.at[9]),
        pltpu.make_async_copy(before, before_v, local_sem.at[1]),
        pltpu.make_async_copy(tables, tables_v, local_sem.at[2]),
        pltpu.make_async_copy(docs, docs_v, local_sem.at[7]),
        pltpu.make_async_copy(after_in, after_v, local_sem.at[8]),
        pltpu.make_async_copy(feed_in, feed_v, local_sem.at[10]),
    ]
    for copy in locals_:
        copy.start()
    wrows, qcols, kcols = wq.shape[0], wq.shape[1], wk.shape[1]
    shard = c if paired else 0
    start = pl.multiple_of(shard * wrows, 16)
    targets = [
        (wq, weights.at[pl.ds(start, wrows), pl.ds(0, qcols)]),
        (wk, weights.at[pl.ds(start, wrows), pl.ds(qcols, kcols)]),
        (wv, weights.at[pl.ds(start, wrows), pl.ds(qcols + kcols, kcols)]),
        (wo, out_weight.at[shard]),
    ]
    weight_local = [
        pltpu.make_async_copy(src, dst, local_sem.at[3 + k]) for k, (src, dst) in enumerate(targets)
    ]

    barrier = pltpu.get_barrier_semaphore()
    greet = [{"hx": along_x}, {"hx": along_y}, {"hx": across}]
    greet += [{"hy": z_peers[j]} for j in (1, 2, 3)]
    if paired:
        greet.append({"tok": 1 - c})
    for peer in greet:
        pl.semaphore_signal(barrier, inc=1, device_id=peer, device_id_type=MESH)
    for copy in weight_local:
        copy.start()

    row8 = lax.broadcasted_iota(jnp.int32, (8, rows), 0)
    for copy in locals_[:3]:
        copy.wait()
    own = jnp.concatenate([slots[0, 0], slots[1, 0]], axis=1).astype(F32)

    def padded(vector):
        wide_vector = vector.astype(F32).reshape(1, width)
        return jnp.concatenate([wide_vector, jnp.zeros((1, rows + LANES - width), F32)], axis=1)

    before_row = padded(before_v[...])
    padded_tail = jnp.concatenate([before_row[:, rows:], jnp.zeros((1, rows - LANES), F32)], axis=1)
    head[...] = jnp.where(
        row8 == 0,
        jnp.sum(own * own, axis=0, keepdims=True),
        jnp.where(row8 == 1, before_row[:, :rows], jnp.where(row8 == 2, padded_tail, 0.0)),
    )
    pl.semaphore_wait(barrier, len(greet))

    def remote(src, dst, send, recv, peer):
        return pltpu.make_async_remote_copy(
            src_ref=src, dst_ref=dst, send_sem=send, recv_sem=recv, device_id=peer, device_id_type=MESH
        )

    def head_to_z(j):
        return remote(head, head_z.at[j - 1], head_send.at[j - 1], head_recv.at[j - 1], {"hy": z_peers[j]})

    def head_to_plane(i):
        return remote(head_mid, head_plane.at[i - 1], head_send.at[2 + i], head_recv.at[2 + i], {"hx": plane[i]})

    def gather(block, h):
        link = GATHER["AB"[h]][4 * block[0] + block[1]]
        origin = parent(block, link)
        k = 4 * block[0] + block[1]
        return remote(
            slots.at[h, 4 * origin[0] + origin[1]], slots.at[h, k], gather_send.at[h, k], gather_recv.at[h, k], peers[link]
        )

    def share(block, h):
        k = 4 * block[0] + block[1]
        link = REDUCE["AB"[h]][k]
        return remote(
            terms.at[h, block[0], pl.ds(within(block[1]), width)], shares.at[h, k],
            reduce_send.at[h, k], reduce_recv.at[h, k], peers[link],
        )

    blocks = [(i, j) for i in range(4) for j in range(4)]
    children = {(h, block): [] for h in range(2) for block in blocks}
    for h in range(2):
        for block in blocks[1:]:
            link = REDUCE["AB"[h]][4 * block[0] + block[1]]
            children[h, parent(block, link)].append(block)

    weight_remote = []
    if paired:
        weight_remote = [
            remote(src, dst, weight_send.at[k], weight_recv.at[k], {"tok": 1 - c})
            for k, (src, dst) in enumerate(targets)
        ]
    state = {}
    arrived = set()

    def await_gather(block, h):
        if block != (0, 0) and ("g", block, h) not in arrived:
            arrived.add(("g", block, h))
            gather(block, h).wait_recv()

    def send_heads():
        for j in (3, 2, 1):
            head_to_z(j).start()

    def send_weights():
        for copy in weight_remote:
            copy.start()

    def relay_heads():
        for j in (1, 2, 3):
            head_to_z(j).wait_recv()
        mains = [head[...]] + [head_z[j] for j in range(3)]
        total = mains[0] + mains[1] + mains[2] + mains[3]
        tails = jnp.zeros((1, rows), F32)
        for j in range(4):
            part = mains[j][2:3, :LANES]
            if j:
                part = pltpu.roll(tall_row(part), j * rest, 1)[0:1]
            tails = tails + jnp.concatenate([part, jnp.zeros((1, rows - LANES), F32)], axis=1)
        mid = jnp.where(row8 == 0, total[0:1], 0.0)
        for j in range(4):
            mid = jnp.where(row8 == 1 + j, mains[j][1:2], mid)
        head_mid[...] = jnp.where(row8 == 5, tails, mid)
        for i in (3, 1, 2):
            head_to_plane(i).start()

    def use_heads():
        for i in (1, 2, 3):
            head_to_plane(i).wait_recv()
        groups = [head_mid[...]] + [head_plane[i] for i in range(3)]
        state["first_sq"] = groups[0][0:1] + groups[1][0:1] + groups[2][0:1] + groups[3][0:1]
        state["first_scale"] = lax.rsqrt(state["first_sq"] / D + epsilon)
        state["gain_columns"] = tall(jnp.concatenate(groups, axis=0))
        for copy in weight_local[:3]:
            copy.wait()
        for copy in weight_remote[:3]:
            copy.wait_recv()

    def normalise(block, h):
        await_gather(block, h)
        i, j = block
        gain_columns = state["gain_columns"]
        gain = jnp.concatenate(
            [gain_columns[:, 8 * i + 1 + j:8 * i + 2 + j], gain_columns[j * rest:(j + 1) * rest, 8 * i + 5:8 * i + 6]],
            axis=0,
        )
        scale = state["first_scale"][:, h * span:(h + 1) * span]
        normed[h, i, pl.ds(within(j), width), :] = (slots[h, 4 * i + j].astype(F32) * scale * gain).astype(BF16)

    def project(i, h):
        part = lax.dot_general(
            weights[pl.ds(group(i), 4 * width), :], normed[h, i], (((0,), (0,)), ((), ())), preferred_element_type=F32
        )
        if ("m", h) not in arrived:
            arrived.add(("m", h))
            acc[h] = part
        else:
            acc[h] += part

    shards, depth, columns = out_weight.shape

    def turn():
        weight_local[3].wait()
        for copy in weight_remote[3:]:
            copy.wait_recv()
        for copy in locals_[3:]:
            copy.wait()
        step = 3 * LANES
        for k in range(D // step):
            s, at = (k * step) // columns, (k * step) % columns
            out_t[k * step:(k + 1) * step, :] = out_weight[s, :, at:at + step].T
        doc_row = docs_v[...].astype(F32)
        after_row = padded(after_v[...])
        state["doc_row"] = doc_row
        state["doc_col"] = tall(jnp.broadcast_to(doc_row, (8, rows)))[:, 0:1]
        feed_row = padded(feed_v[...])
        state["feed"] = tall(jnp.broadcast_to(feed_row, (8, rows + LANES)))[:width, 0:1]
        state["after"] = tall(jnp.broadcast_to(after_row, (8, rows + LANES)))[:width, 0:1]

    query_heads, key_heads = qcols // HEAD, kcols // HEAD
    ratio = query_heads // key_heads

    def attend(h):
        lanes = slice(h * span, (h + 1) * span)
        seen = (h + 1) * span
        cosine, sine = tables_v[0, :, lanes], tables_v[1, :, lanes]

        def rope(x):
            upper, lower = x[:HEAD // 2], x[HEAD // 2:]
            return jnp.concatenate([upper * cosine - lower * sine, lower * cosine + upper * sine], axis=0)

        for kv in range(key_heads):
            keys[kv, :, lanes] = rope(acc[h, qcols + kv * HEAD:qcols + (kv + 1) * HEAD]).astype(BF16)
            values[kv, :, lanes] = acc[h, qcols + kcols + kv * HEAD:qcols + kcols + (kv + 1) * HEAD].astype(BF16)
        s_index = lax.broadcasted_iota(jnp.int32, (seen, span), 0)
        t_index = lax.broadcasted_iota(jnp.int32, (seen, span), 1) + h * span
        allowed = (s_index <= t_index) & (state["doc_row"][:, lanes] == state["doc_col"][:seen])
        for q in range(query_heads):
            query = (rope(acc[h, q * HEAD:(q + 1) * HEAD]) * (D / QH) ** (-0.5)).astype(BF16)
            key, value = keys[q // ratio, :, :seen], values[q // ratio, :, :seen]
            scores = lax.dot_general(key, query, (((0,), (0,)), ((), ())), preferred_element_type=F32)
            best = jnp.max(jnp.where(allowed, scores, neg_big), axis=0, keepdims=True)
            soft = jnp.where(allowed, jnp.exp(scores - best), 0.0)
            mass = jnp.sum(soft, axis=0, keepdims=True)
            blended = jnp.dot(value, soft.astype(BF16), preferred_element_type=F32)
            attended[h, q * HEAD:(q + 1) * HEAD, :] = (blended / mass).astype(BF16)

    def term(i, h):
        terms[h, i] = jnp.dot(
            out_t[pl.ds(group(i), 4 * width), :], attended[h], preferred_element_type=F32
        ).astype(BF16)

    def collect(block, h):
        for child in children[h, block]:
            share(child, h).wait_recv()
        total = terms[h, block[0], pl.ds(within(block[1]), width), :].astype(F32)
        for child in children[h, block]:
            total = total + shares[h, 4 * child[0] + child[1]].astype(F32)
        return total

    def pass_on(block, h):
        if children[h, block]:
            terms[h, block[0], pl.ds(within(block[1]), width), :] = collect(block, h).astype(BF16)
        share(block, h).start()

    def finish(h):
        mixed = collect((0, 0), h)
        lanes = slice(h * span, (h + 1) * span)
        wide = slots[h, 0].astype(F32)
        branch = mixed * state["after"]
        narrow = row8[:, :span]
        stats[:, lanes] = jnp.where(
            narrow == 0,
            jnp.sum(mixed * mixed, axis=0, keepdims=True),
            jnp.where(
                narrow == 1,
                jnp.sum(wide * branch, axis=0, keepdims=True),
                jnp.sum(branch * branch, axis=0, keepdims=True),
            ),
        )
        branch_v[:, lanes] = branch

    for task in ORDER:
        if task == "hz":
            send_heads()
        elif task == "hw":
            send_weights()
        elif task == "hm":
            relay_heads()
        elif task == "head":
            use_heads()
        elif task == "turn":
            turn()
        elif task[:3] == "fin":
            finish("AB".index(task[3]))
        elif task[0] == "a":
            attend("AB".index(task[1]))
        elif task[0] == "m":
            project(int(task[1]), "AB".index(task[2]))
        elif task[0] == "t":
            term(int(task[1]), "AB".index(task[2]))
        else:
            block, h = (int(task[1]), int(task[2])), "AB".index(task[3])
            if task[0] == "s":
                await_gather(parent(block, GATHER["AB"[h]][4 * block[0] + block[1]]), h)
                gather(block, h).start()
            elif task[0] == "n":
                normalise(block, h)
            else:
                pass_on(block, h)

    def stat_plane(i):
        return remote(stats, stats_in.at[i - 1], stat_send.at[i - 1], stat_recv.at[i - 1], {"hx": plane[i]})

    def stat_z(j):
        return remote(stats_mid, stats_zin.at[j - 1], stat_send.at[2 + j], stat_recv.at[2 + j], {"hy": z_peers[j]})

    for i in (3, 2, 1):
        stat_plane(i).start()
    for i in (1, 2, 3):
        stat_plane(i).wait_recv()
    stats_mid[...] = stats[...] + stats_in[0] + stats_in[1] + stats_in[2]
    for j in (3, 2, 1):
        stat_z(j).start()
    for h in range(2):
        for block in blocks[1:]:
            gather(block, h).wait_send()
            share(block, h).wait_send()
    for j in (1, 2, 3):
        head_to_z(j).wait_send()
        head_to_plane(j).wait_send()
        stat_plane(j).wait_send()
    for copy in weight_remote:
        copy.wait_send()
    for j in (1, 2, 3):
        stat_z(j).wait_recv()
    summed = stats_mid[...] + stats_zin[0] + stats_zin[1] + stats_zin[2]
    after_scale = lax.rsqrt(summed[0:1] / D + epsilon)
    feed_sq = state["first_sq"] + 2.0 * after_scale * summed[1:2] + after_scale * after_scale * summed[2:3]
    feed_scale = lax.rsqrt(feed_sq / D + epsilon)
    for h in range(2):
        lanes = slice(h * span, (h + 1) * span)
        residual = (slots[h, 0].astype(F32) + branch_v[:, lanes] * after_scale[:, lanes]).astype(BF16)
        outs[0, :, lanes] = residual
        outs[1, :, lanes] = (residual.astype(F32) * feed_scale[:, lanes] * state["feed"]).astype(BF16)
    for j in (1, 2, 3):
        stat_z(j).wait_send()


def per_device(paired, stream_in, before_gain, after_gain, feed_gain, query_weight, key_weight, value_weight, output_weight, documents):
    rows, width = stream_in.shape
    if not paired:
        query_weight, key_weight, value_weight = (
            lax.all_gather(piece, "tok", axis=0, tiled=True) for piece in (query_weight, key_weight, value_weight)
        )
        output_weight = lax.all_gather(output_weight, "tok", axis=1, tiled=True)
    tables = jnp.asarray(rope_tables())
    qcols, kcols = query_weight.shape[1], key_weight.shape[1]
    shards = 2 if paired else 1
    depth = output_weight.shape[0]
    any_spec = pl.BlockSpec(memory_space=pl.ANY)
    vmem = pl.BlockSpec(memory_space=pltpu.VMEM)
    dma = pltpu.SemaphoreType.DMA
    block, piece = (width, rows), (width, rows // 2)
    both = pl.pallas_call(
        functools.partial(kernel, paired),
        out_shape=jax.ShapeDtypeStruct((2,) + block, BF16),
        in_specs=[any_spec] * 10,
        out_specs=vmem,
        scratch_shapes=[
            pltpu.VMEM((2, 16) + piece, BF16),
            pltpu.VMEM((1, rows), jnp.int32),
            pltpu.VMEM((width,), BF16),
            pltpu.VMEM((width,), BF16),
            pltpu.VMEM((width,), BF16),
            pltpu.VMEM(block, F32),
            pltpu.VMEM((2, HEAD // 2, LENGTH), F32),
            pltpu.VMEM((D, qcols + 2 * kcols), BF16),
            pltpu.VMEM((shards, depth, output_weight.shape[1]), BF16),
            pltpu.VMEM((D, depth), BF16),
            pltpu.VMEM((2, qcols + 2 * kcols, rows // 2), F32),
            pltpu.VMEM((kcols // HEAD, HEAD, rows), BF16),
            pltpu.VMEM((kcols // HEAD, HEAD, rows), BF16),
            pltpu.VMEM((2, qcols, rows // 2), BF16),
            pltpu.VMEM((2, 4, 4 * width, rows // 2), BF16),
            pltpu.VMEM((2, 4, 4 * width, rows // 2), BF16),
            pltpu.VMEM((2, 16) + piece, BF16),
        ]
        + [pltpu.VMEM((8, rows), F32), pltpu.VMEM((3, 8, rows), F32)] * 4
        + [
            dma((11,)),
            dma((4,)),
            dma((4,)),
            dma((2, 16)),
            dma((2, 16)),
            dma((2, 16)),
            dma((2, 16)),
            dma((6,)),
            dma((6,)),
            dma((6,)),
            dma((6,)),
        ],
        compiler_params=pltpu.CompilerParams(
            collective_id=0, has_side_effects=True, vmem_limit_bytes=56 * 1024 * 1024
        ),
    )(
        stream_in.T,
        documents.reshape(1, rows),
        before_gain,
        after_gain,
        feed_gain,
        tables,
        query_weight,
        key_weight,
        value_weight,
        output_weight,
    )
    return both[0].T, both[1].T


def solution(mesh):
    both = ("hx", "hy")
    in_specs = (
        P("tok", both),
        P(both),
        P(both),
        P(both),
        P("tok", both),
        P("tok", both),
        P("tok", both),
        P(both, "tok"),
        P("tok"),
    )
    out_specs = (P("tok", both), P("tok", both))
    paired = mesh.shape["tok"] == 2
    return jax.shard_map(
        functools.partial(per_device, paired), mesh=mesh, in_specs=in_specs, out_specs=out_specs, check_vma=False
    )
```

```python
import functools

import jax
import jax.numpy as jnp
import numpy as np
from jax import lax
from jax.experimental import pallas as pl
from jax.experimental.pallas import tpu as pltpu
from jax.sharding import PartitionSpec as P

D = 4608
QH = 32
HEAD = 128
LENGTH = 256
LANES = 128

epsilon = 1e-06
neg_big = -1e30
MESH = pl.DeviceIdType.MESH
F32 = jnp.float32
BF16 = jnp.bfloat16


PIECES = 1
GATHER = {
    "A": ("", "z1", "z2", "z1", "x", "x", "x", "z1", "y", "y", "y", "y", "d", "x", "x", "y"),
    "B": ("", "z1", "z2", "z1", "x", "z1", "x", "z1", "y", "z1", "y", "z1", "d", "x", "y", "d"),
}
REDUCE = {
    "A": ("", "z1", "z2", "z3", "x", "z1", "x", "x", "y", "z1", "y", "y", "x", "y", "z1", "d"),
    "B": ("", "z1", "z2", "z1", "x", "x", "x", "x", "y", "y", "y", "y", "d", "z1", "d", "z1"),
}
ORDER = (
    "s02A", "s10B", "s20A", "hz", "s01A", "s02B", "s10A", "s30B", "s30A", "s20B", "s03A", "s12A",
    "s22A", "w0", "hw", "hm", "s21B", "s11A", "s21A", "s12B", "s13A", "s03B", "s23A", "s32A",
    "head", "w1", "n00A", "s11B", "n30B", "n10B", "n02A", "s22B", "n11A", "turn", "s31A", "n20A",
    "n12A", "s33A", "s01B", "n21A", "n23A", "n01A", "n03A", "n13A", "s32B", "m0A", "s31B", "n10A",
    "n03B", "s33B", "n12B", "n22A", "n32A", "s23B", "n22B", "m1A", "m2A", "n02B", "s13B", "n31A",
    "n11B", "n21B", "n00B", "n20B", "n30A", "n33A", "m3A", "aA", "t3A", "u32A", "u31A", "u30A",
    "t2A", "u22A", "n32B", "t1A", "t0A", "n31B", "n23B", "u01A", "u12A", "m2B", "n01B", "m0B",
    "u23A", "u13A", "u21A", "n33B", "n13B", "m3B", "m1B", "aB", "t3B", "u33B", "u33A", "u11A",
    "u31B", "u02A", "t1B", "t2B", "u13B", "u12B", "u23B", "u22B", "t0B", "u32B", "u11B", "u03B",
    "u03A", "u10A", "u10B", "u21B", "u20A", "u02B", "u20B", "u30B", "u01B", "finA", "finB",
)


def flip(index, mask):
    low = (index % 2 + mask % 2) % 2
    high = (index // 2 + mask // 2) % 2
    return low + 2 * high


def rope_tables():
    half = HEAD // 2
    frequency = (10000.0 ** (-np.arange(half, dtype=np.float32) / half)).astype(np.float32)
    angles = frequency[:, None] * np.arange(LENGTH, dtype=np.float32)[None, :]
    return np.stack([np.cos(angles), np.sin(angles)]).astype(np.float32)


def tall_row(row):
    return jnp.broadcast_to(row, (8, row.shape[1]))


def tall(block):
    return jnp.concatenate([block] * (LANES // block.shape[0]), axis=0).T


def parent(block, link):
    i, j = block
    if link == "x":
        return i ^ 1, j
    if link == "y":
        return i ^ 2, j
    if link == "d":
        return i ^ 3, j
    return i, j ^ int(link[1])


def kernel(
    paired,
    stream, docs, before, after_in, feed_in, tables, wq, wk, wv, wo,
    outs,
    slots, docs_v, before_v, after_v, feed_v, branch_v, tables_v, weights, weights_t, out_weight, out_t, acc, keys, values, attended,
    normed, terms, shares, head, head_z, head_mid, head_plane, stats, stats_in,
    local_sem, weight_send, weight_recv, gather_send, gather_recv, reduce_send, reduce_recv,
    head_send, head_recv, stat_send, stat_recv,
):
    width, rows = stream.shape
    rest = width - rows
    span = rows // 2
    a, b, c = lax.axis_index("hx"), lax.axis_index("hy"), lax.axis_index("tok")
    along_x, along_y, across = flip(a, 1), flip(a, 2), flip(a, 3)
    plane = (None, along_x, along_y, across)
    z_peers = [None] + [flip(b, j) for j in (1, 2, 3)]
    peers = {"x": {"hx": along_x}, "y": {"hx": along_y}, "d": {"hx": across}}
    for j in (1, 2, 3):
        peers["z" + str(j)] = {"hy": z_peers[j]}

    def group(i):
        return pl.multiple_of(flip(a, i) * (4 * width), LANES)

    def within(j):
        return pl.multiple_of(flip(b, j) * width, 16)

    locals_ = [
        pltpu.make_async_copy(stream.at[:, pl.ds(0, span)], slots.at[0, 0], local_sem.at[0]),
        pltpu.make_async_copy(stream.at[:, pl.ds(span, span)], slots.at[1, 0], local_sem.at[9]),
        pltpu.make_async_copy(before, before_v, local_sem.at[1]),
        pltpu.make_async_copy(tables, tables_v, local_sem.at[2]),
        pltpu.make_async_copy(docs, docs_v, local_sem.at[7]),
        pltpu.make_async_copy(after_in, after_v, local_sem.at[8]),
        pltpu.make_async_copy(feed_in, feed_v, local_sem.at[10]),
    ]
    for copy in locals_:
        copy.start()
    wrows, qcols, kcols = wq.shape[0], wq.shape[1], wk.shape[1]
    shard = c if paired else 0
    start = pl.multiple_of(shard * wrows, LANES)
    targets = [
        (wq, weights.at[pl.ds(start, wrows), pl.ds(0, qcols)]),
        (wk, weights.at[pl.ds(start, wrows), pl.ds(qcols, kcols)]),
        (wv, weights.at[pl.ds(start, wrows), pl.ds(qcols + kcols, kcols)]),
        (wo, out_weight.at[shard]),
    ]
    weight_local = [
        pltpu.make_async_copy(src, dst, local_sem.at[3 + k]) for k, (src, dst) in enumerate(targets)
    ]

    barrier = pltpu.get_barrier_semaphore()
    greet = [{"hx": along_x}, {"hx": along_y}, {"hx": across}]
    greet += [{"hy": z_peers[j]} for j in (1, 2, 3)]
    if paired:
        greet.append({"tok": 1 - c})
    for peer in greet:
        pl.semaphore_signal(barrier, inc=1, device_id=peer, device_id_type=MESH)
    for copy in weight_local:
        copy.start()

    row8 = lax.broadcasted_iota(jnp.int32, (8, rows), 0)
    for copy in locals_[:3]:
        copy.wait()
    own = jnp.concatenate([slots[0, 0], slots[1, 0]], axis=1).astype(F32)

    def padded(vector):
        wide_vector = vector.astype(F32).reshape(1, width)
        return jnp.concatenate([wide_vector, jnp.zeros((1, rows + LANES - width), F32)], axis=1)

    before_row = padded(before_v[...])
    padded_tail = jnp.concatenate([before_row[:, rows:], jnp.zeros((1, rows - LANES), F32)], axis=1)
    head[...] = jnp.where(
        row8 == 0,
        jnp.sum(own * own, axis=0, keepdims=True),
        jnp.where(row8 == 1, before_row[:, :rows], jnp.where(row8 == 2, padded_tail, 0.0)),
    )
    pl.semaphore_wait(barrier, len(greet))

    def remote(src, dst, send, recv, peer):
        return pltpu.make_async_remote_copy(
            src_ref=src, dst_ref=dst, send_sem=send, recv_sem=recv, device_id=peer, device_id_type=MESH
        )

    def head_to_z(j):
        return remote(head, head_z.at[j - 1], head_send.at[j - 1], head_recv.at[j - 1], {"hy": z_peers[j]})

    def head_to_plane(i):
        return remote(head_mid, head_plane.at[i - 1], head_send.at[2 + i], head_recv.at[2 + i], {"hx": plane[i]})

    count = gather_send.shape[2]
    part = width // count

    def gather(block, h, f):
        link = GATHER["AB"[h]][4 * block[0] + block[1]]
        origin = parent(block, link)
        k, rows_of = 4 * block[0] + block[1], pl.ds(f * part, part)
        return remote(
            slots.at[h, 4 * origin[0] + origin[1], rows_of], slots.at[h, k, rows_of],
            gather_send.at[h, k, f], gather_recv.at[h, k, f], peers[link],
        )

    def piece_of(block, f):
        return pl.ds(pl.multiple_of(within(block[1]) + f * part, 16), part)

    def share(block, h, f):
        k = 4 * block[0] + block[1]
        link = REDUCE["AB"[h]][k]
        return remote(
            terms.at[h, block[0], piece_of(block, f)], shares.at[h, k, pl.ds(f * part, part)],
            reduce_send.at[h, k, f], reduce_recv.at[h, k, f], peers[link],
        )

    blocks = [(i, j) for i in range(4) for j in range(4)]
    children = {(h, block): [] for h in range(2) for block in blocks}
    for h in range(2):
        for block in blocks[1:]:
            link = REDUCE["AB"[h]][4 * block[0] + block[1]]
            children[h, parent(block, link)].append(block)

    weight_remote = []
    if paired:
        weight_remote = [
            remote(src, dst, weight_send.at[k], weight_recv.at[k], {"tok": 1 - c})
            for k, (src, dst) in enumerate(targets)
        ]
    state = {}
    arrived = set()

    def await_gather(block, h, f):
        if block != (0, 0) and ("g", block, h, f) not in arrived:
            arrived.add(("g", block, h, f))
            gather(block, h, f).wait_recv()

    def send_heads():
        for j in (3, 2, 1):
            head_to_z(j).start()

    def send_weights():
        for copy in weight_remote:
            copy.start()

    def relay_heads():
        for j in (1, 2, 3):
            head_to_z(j).wait_recv()
        mains = [head[...]] + [head_z[j] for j in range(3)]
        total = mains[0] + mains[1] + mains[2] + mains[3]
        tails = jnp.zeros((1, rows), F32)
        for j in range(4):
            part = mains[j][2:3, :LANES]
            if j:
                part = pltpu.roll(tall_row(part), j * rest, 1)[0:1]
            tails = tails + jnp.concatenate([part, jnp.zeros((1, rows - LANES), F32)], axis=1)
        mid = jnp.where(row8 == 0, total[0:1], 0.0)
        for j in range(4):
            mid = jnp.where(row8 == 1 + j, mains[j][1:2], mid)
        head_mid[...] = jnp.where(row8 == 5, tails, mid)
        for i in (3, 1, 2):
            head_to_plane(i).start()

    def use_heads():
        for i in (1, 2, 3):
            head_to_plane(i).wait_recv()
        groups = [head_mid[...]] + [head_plane[i] for i in range(3)]
        state["first_sq"] = groups[0][0:1] + groups[1][0:1] + groups[2][0:1] + groups[3][0:1]
        state["first_scale"] = lax.rsqrt(state["first_sq"] / D + epsilon)
        state["gain_columns"] = tall(jnp.concatenate(groups, axis=0))

    def turn_weights(first, amount):
        for k in range(amount // (4 * width)):
            at = pl.ds(pl.multiple_of(first + k * 4 * width, LANES), 4 * width)
            weights_t[:, at] = weights[at, :].T

    def own_weights():
        for copy in weight_local[:3]:
            copy.wait()
        turn_weights(start, wrows)

    def other_weights():
        for copy in weight_remote[:3]:
            copy.wait_recv()
        if paired:
            turn_weights(pl.multiple_of((1 - c) * wrows, LANES), wrows)

    def normalise(block, h):
        for f in range(count):
            await_gather(block, h, f)
        i, j = block
        gain_columns = state["gain_columns"]
        gain = jnp.concatenate(
            [gain_columns[:, 8 * i + 1 + j:8 * i + 2 + j], gain_columns[j * rest:(j + 1) * rest, 8 * i + 5:8 * i + 6]],
            axis=0,
        )
        scale = state["first_scale"][:, h * span:(h + 1) * span]
        normed[h, i, pl.ds(within(j), width), :] = (slots[h, 4 * i + j].astype(F32) * scale * gain).astype(BF16)

    def project(i, h):
        product = jnp.dot(weights_t[:, pl.ds(group(i), 4 * width)], normed[h, i], preferred_element_type=F32)
        if ("m", h) not in arrived:
            arrived.add(("m", h))
            acc[h] = product
        else:
            acc[h] += product

    shards, depth, columns = out_weight.shape

    def turn():
        weight_local[3].wait()
        for copy in weight_remote[3:]:
            copy.wait_recv()
        for copy in locals_[3:]:
            copy.wait()
        step = 3 * LANES
        for k in range(D // step):
            s, at = (k * step) // columns, (k * step) % columns
            out_t[k * step:(k + 1) * step, :] = out_weight[s, :, at:at + step].T
        doc_row = docs_v[...].astype(F32)
        after_row = padded(after_v[...])
        state["doc_row"] = doc_row
        state["doc_col"] = tall(jnp.broadcast_to(doc_row, (8, rows)))[:, 0:1]
        feed_row = padded(feed_v[...])
        state["feed"] = tall(jnp.broadcast_to(feed_row, (8, rows + LANES)))[:width, 0:1]
        state["after"] = tall(jnp.broadcast_to(after_row, (8, rows + LANES)))[:width, 0:1]

    query_heads, key_heads = qcols // HEAD, kcols // HEAD
    ratio = query_heads // key_heads

    def attend(h):
        lanes = slice(h * span, (h + 1) * span)
        seen = (h + 1) * span
        cosine, sine = tables_v[0, :, lanes], tables_v[1, :, lanes]

        def rope(x):
            upper, lower = x[:HEAD // 2], x[HEAD // 2:]
            return jnp.concatenate([upper * cosine - lower * sine, lower * cosine + upper * sine], axis=0)

        for kv in range(key_heads):
            keys[kv, :, lanes] = rope(acc[h, qcols + kv * HEAD:qcols + (kv + 1) * HEAD]).astype(BF16)
            values[kv, :, lanes] = acc[h, qcols + kcols + kv * HEAD:qcols + kcols + (kv + 1) * HEAD].astype(BF16)
        s_index = lax.broadcasted_iota(jnp.int32, (seen, span), 0)
        t_index = lax.broadcasted_iota(jnp.int32, (seen, span), 1) + h * span
        allowed = (s_index <= t_index) & (state["doc_row"][:, lanes] == state["doc_col"][:seen])
        for q in range(query_heads):
            query = (rope(acc[h, q * HEAD:(q + 1) * HEAD]) * (D / QH) ** (-0.5)).astype(BF16)
            key, value = keys[q // ratio, :, :seen], values[q // ratio, :, :seen]
            scores = lax.dot_general(key, query, (((0,), (0,)), ((), ())), preferred_element_type=F32)
            best = jnp.max(jnp.where(allowed, scores, neg_big), axis=0, keepdims=True)
            soft = jnp.where(allowed, jnp.exp(scores - best), 0.0)
            mass = jnp.sum(soft, axis=0, keepdims=True)
            blended = jnp.dot(value, soft.astype(BF16), preferred_element_type=F32)
            attended[h, q * HEAD:(q + 1) * HEAD, :] = (blended / mass).astype(BF16)

    def term(i, h):
        terms[h, i] = jnp.dot(
            out_t[pl.ds(group(i), 4 * width), :], attended[h], preferred_element_type=F32
        ).astype(BF16)

    def collect(block, h, f):
        for child in children[h, block]:
            share(child, h, f).wait_recv()
        total = terms[h, block[0], piece_of(block, f), :].astype(F32)
        for child in children[h, block]:
            total = total + shares[h, 4 * child[0] + child[1], f * part:(f + 1) * part].astype(F32)
        return total

    def pass_on(block, h, f):
        if children[h, block]:
            terms[h, block[0], piece_of(block, f), :] = collect(block, h, f).astype(BF16)
        share(block, h, f).start()

    def finish(h):
        lanes = slice(h * span, (h + 1) * span)
        sums = [0.0, 0.0, 0.0]
        for f in range(count):
            mixed = collect((0, 0), h, f)
            at = slice(f * part, (f + 1) * part)
            branch = mixed * state["after"][at]
            branch_v[at, lanes] = branch
            for k, product in enumerate((mixed * mixed, slots[h, 0, at].astype(F32) * branch, branch * branch)):
                sums[k] = sums[k] + jnp.sum(product, axis=0, keepdims=True)
        row4 = lax.broadcasted_iota(jnp.int32, (4, span), 0)
        stats[4 * h:4 * h + 4, :] = jnp.where(row4 == 0, sums[0], jnp.where(row4 == 1, sums[1], sums[2]))

    for task in ORDER:
        if task == "hz":
            send_heads()
        elif task == "hw":
            send_weights()
        elif task == "w0":
            own_weights()
        elif task == "w1":
            other_weights()
        elif task == "hm":
            relay_heads()
        elif task == "head":
            use_heads()
        elif task == "turn":
            turn()
        elif task[:3] == "fin":
            finish("AB".index(task[3]))
        elif task[0] == "a":
            attend("AB".index(task[1]))
        elif task[0] == "m":
            project(int(task[1]), "AB".index(task[2]))
        elif task[0] == "t":
            term(int(task[1]), "AB".index(task[2]))
        else:
            block, h = (int(task[1]), int(task[2])), "AB".index(task[3])
            f = int(task[4]) if len(task) > 4 else 0
            if task[0] == "s":
                await_gather(parent(block, GATHER["AB"[h]][4 * block[0] + block[1]]), h, f)
                gather(block, h, f).start()
            elif task[0] == "n":
                normalise(block, h)
            else:
                pass_on(block, h, f)

    def stat(i, j):
        k = 4 * i + j
        return remote(
            stats, stats_in.at[k], stat_send.at[k], stat_recv.at[k], {"hx": flip(a, i), "hy": flip(b, j)}
        )

    far_first = sorted(blocks[1:], key=lambda block: -(bin(block[0]).count("1") + block[1]))
    for block in far_first:
        stat(*block).start()
    for h in range(2):
        for block in blocks[1:]:
            for f in range(count):
                gather(block, h, f).wait_send()
                share(block, h, f).wait_send()
    for j in (1, 2, 3):
        head_to_z(j).wait_send()
        head_to_plane(j).wait_send()
    for copy in weight_remote:
        copy.wait_send()
    packed = stats[...]
    for block in reversed(far_first):
        stat(*block).wait_recv()
        packed = packed + stats_in[4 * block[0] + block[1]]
    summed = jnp.concatenate([packed[0:3], packed[4:7]], axis=1)
    after_scale = lax.rsqrt(summed[0:1] / D + epsilon)
    feed_sq = state["first_sq"] + 2.0 * after_scale * summed[1:2] + after_scale * after_scale * summed[2:3]
    feed_scale = lax.rsqrt(feed_sq / D + epsilon)
    for h in range(2):
        lanes = slice(h * span, (h + 1) * span)
        residual = (slots[h, 0].astype(F32) + branch_v[:, lanes] * after_scale[:, lanes]).astype(BF16)
        outs[0, :, lanes] = residual
        outs[1, :, lanes] = (residual.astype(F32) * feed_scale[:, lanes] * state["feed"]).astype(BF16)
    for block in far_first:
        stat(*block).wait_send()


def per_device(paired, stream_in, before_gain, after_gain, feed_gain, query_weight, key_weight, value_weight, output_weight, documents):
    rows, width = stream_in.shape
    if not paired:
        query_weight, key_weight, value_weight = (
            lax.all_gather(piece, "tok", axis=0, tiled=True) for piece in (query_weight, key_weight, value_weight)
        )
        output_weight = lax.all_gather(output_weight, "tok", axis=1, tiled=True)
    tables = jnp.asarray(rope_tables())
    qcols, kcols = query_weight.shape[1], key_weight.shape[1]
    shards = 2 if paired else 1
    depth = output_weight.shape[0]
    any_spec = pl.BlockSpec(memory_space=pl.ANY)
    vmem = pl.BlockSpec(memory_space=pltpu.VMEM)
    dma = pltpu.SemaphoreType.DMA
    block, piece = (width, rows), (width, rows // 2)
    both = pl.pallas_call(
        functools.partial(kernel, paired),
        out_shape=pltpu.VMEM((2,) + block, BF16),
        in_specs=[any_spec] * 10,
        out_specs=vmem,
        scratch_shapes=[
            pltpu.VMEM((2, 16) + piece, BF16),
            pltpu.VMEM((1, rows), jnp.int32),
            pltpu.VMEM((width,), BF16),
            pltpu.VMEM((width,), BF16),
            pltpu.VMEM((width,), BF16),
            pltpu.VMEM(block, F32),
            pltpu.VMEM((2, HEAD // 2, LENGTH), F32),
            pltpu.VMEM((D, qcols + 2 * kcols), BF16),
            pltpu.VMEM((qcols + 2 * kcols, D), BF16),
            pltpu.VMEM((shards, depth, output_weight.shape[1]), BF16),
            pltpu.VMEM((D, depth), BF16),
            pltpu.VMEM((2, qcols + 2 * kcols, rows // 2), F32),
            pltpu.VMEM((kcols // HEAD, HEAD, rows), BF16),
            pltpu.VMEM((kcols // HEAD, HEAD, rows), BF16),
            pltpu.VMEM((2, qcols, rows // 2), BF16),
            pltpu.VMEM((2, 4, 4 * width, rows // 2), BF16),
            pltpu.VMEM((2, 4, 4 * width, rows // 2), BF16),
            pltpu.VMEM((2, 16) + piece, BF16),
        ]
        + [pltpu.VMEM((8, rows), F32), pltpu.VMEM((3, 8, rows), F32)] * 2
        + [pltpu.VMEM((8, rows // 2), F32), pltpu.VMEM((16, 8, rows // 2), F32)]
        + [
            dma((11,)),
            dma((4,)),
            dma((4,)),
            dma((2, 16, PIECES)),
            dma((2, 16, PIECES)),
            dma((2, 16, PIECES)),
            dma((2, 16, PIECES)),
            dma((6,)),
            dma((6,)),
            dma((16,)),
            dma((16,)),
        ],
        compiler_params=pltpu.CompilerParams(
            collective_id=0, has_side_effects=True, vmem_limit_bytes=56 * 1024 * 1024
        ),
    )(
        stream_in.T,
        documents.reshape(1, rows),
        before_gain,
        after_gain,
        feed_gain,
        tables,
        query_weight,
        key_weight,
        value_weight,
        output_weight,
    )
    return both[0].T, both[1].T


def solution(mesh):
    both = ("hx", "hy")
    in_specs = (
        P("tok", both),
        P(both),
        P(both),
        P(both),
        P("tok", both),
        P("tok", both),
        P("tok", both),
        P(both, "tok"),
        P("tok"),
    )
    out_specs = (P("tok", both), P("tok", both))
    paired = mesh.shape["tok"] == 2
    return jax.shard_map(
        functools.partial(per_device, paired), mesh=mesh, in_specs=in_specs, out_specs=out_specs, check_vma=False
    )
```

```python
import functools

import jax
import jax.numpy as jnp
import numpy as np
from jax import lax
from jax.experimental import pallas as pl
from jax.experimental.pallas import tpu as pltpu
from jax.sharding import PartitionSpec as P

D = 4608
QH = 32
HEAD = 128
LENGTH = 256
LANES = 128

epsilon = 1e-06
neg_big = -1e30
MESH = pl.DeviceIdType.MESH
F32 = jnp.float32
BF16 = jnp.bfloat16


PIECES = 1
GATHER = {
    "A": ("", "z1", "z2", "z1", "x", "x", "x", "z1", "y", "y", "y", "y", "d", "x", "x", "y"),
    "B": ("", "z1", "z2", "z1", "x", "z1", "x", "z1", "y", "z1", "y", "z1", "d", "x", "y", "d"),
}
REDUCE = {
    "A": ("", "z1", "z2", "z3", "x", "z1", "x", "x", "y", "z1", "y", "y", "x", "y", "z1", "d"),
    "B": ("", "z1", "z2", "z1", "x", "x", "x", "x", "y", "y", "y", "y", "d", "z1", "d", "z1"),
}
ORDER = (
    "s02A", "s10B", "s20A", "hz", "hw", "s01A", "s02B", "s10A", "s30B", "s30A", "s20B", "s03A",
    "s12A", "s22A", "w0", "hm", "s21B", "s11A", "s21A", "s13A", "s12B", "s03B", "s23A", "s32A",
    "head", "w1", "n00A", "s11B", "n30B", "n10B", "n02A", "s22B", "n11A", "turn", "s31A", "n20A",
    "n12A", "s33A", "s01B", "n21A", "n23A", "n01A", "n03A", "n13A", "s32B", "m0A", "s31B", "n10A",
    "n03B", "n32A", "s23B", "s33B", "n12B", "n22A", "n22B", "m1A", "m2A", "n02B", "s13B", "n31A",
    "n11B", "n21B", "n00B", "n20B", "n30A", "n33A", "m3A", "aA", "t3A", "u32A", "u31A", "u30A",
    "t2A", "u22A", "n32B", "t1A", "t0A", "n31B", "n23B", "u01A", "u12A", "m2B", "n01B", "m0B",
    "u23A", "u13A", "u21A", "n33B", "n13B", "m3B", "m1B", "aB", "t3B", "u33B", "u33A", "u11A",
    "u31B", "u02A", "t1B", "t2B", "u13B", "u12B", "u23B", "u22B", "u32B", "t0B", "u11B", "u03B",
    "u03A", "u10A", "u10B", "u21B", "u20A", "u02B", "u20B", "u30B", "u01B", "finA", "finB",
)


def flip(index, mask):
    low = (index % 2 + mask % 2) % 2
    high = (index // 2 + mask // 2) % 2
    return low + 2 * high


def rope_tables():
    half = HEAD // 2
    frequency = (10000.0 ** (-np.arange(half, dtype=np.float32) / half)).astype(np.float32)
    angles = frequency[:, None] * np.arange(LENGTH, dtype=np.float32)[None, :]
    return np.stack([np.cos(angles), np.sin(angles)]).astype(np.float32)


def tall_row(row):
    return jnp.broadcast_to(row, (8, row.shape[1]))


def tall(block):
    return jnp.concatenate([block] * (LANES // block.shape[0]), axis=0).T


def parent(block, link):
    i, j = block
    if link == "x":
        return i ^ 1, j
    if link == "y":
        return i ^ 2, j
    if link == "d":
        return i ^ 3, j
    return i, j ^ int(link[1])


def kernel(
    paired,
    stream, docs, before, after_in, feed_in, tables, wq, wk, wv, wo,
    outs,
    slots, docs_v, before_v, after_v, feed_v, branch_v, tables_v, weights, weights_t, out_weight, out_t, acc, keys, values, attended,
    normed, terms, shares, head, head_z, head_mid, head_plane, stats, stats_in,
    local_sem, send_sem, weight_recv, gather_recv, reduce_recv, head_recv, stat_recv,
):
    width, rows = stream.shape
    rest = width - rows
    span = rows // 2
    a, b, c = lax.axis_index("hx"), lax.axis_index("hy"), lax.axis_index("tok")
    along_x, along_y, across = flip(a, 1), flip(a, 2), flip(a, 3)
    plane = (None, along_x, along_y, across)
    z_peers = [None] + [flip(b, j) for j in (1, 2, 3)]
    peers = {"x": {"hx": along_x}, "y": {"hx": along_y}, "d": {"hx": across}}
    for j in (1, 2, 3):
        peers["z" + str(j)] = {"hy": z_peers[j]}

    def group(i):
        return pl.multiple_of(flip(a, i) * (4 * width), LANES)

    def within(j):
        return pl.multiple_of(flip(b, j) * width, 16)

    locals_ = [
        pltpu.make_async_copy(stream.at[:, pl.ds(0, span)], slots.at[0, 0], local_sem.at[0]),
        pltpu.make_async_copy(stream.at[:, pl.ds(span, span)], slots.at[1, 0], local_sem.at[9]),
        pltpu.make_async_copy(before, before_v, local_sem.at[1]),
        pltpu.make_async_copy(tables, tables_v, local_sem.at[2]),
        pltpu.make_async_copy(docs, docs_v, local_sem.at[7]),
        pltpu.make_async_copy(after_in, after_v, local_sem.at[8]),
        pltpu.make_async_copy(feed_in, feed_v, local_sem.at[10]),
    ]
    for copy in locals_:
        copy.start()
    wrows, qcols, kcols = wq.shape[0], wq.shape[1], wk.shape[1]
    shard = c if paired else 0
    start = pl.multiple_of(shard * wrows, LANES)
    targets = [
        (wq, weights.at[pl.ds(start, wrows), pl.ds(0, qcols)]),
        (wk, weights.at[pl.ds(start, wrows), pl.ds(qcols, kcols)]),
        (wv, weights.at[pl.ds(start, wrows), pl.ds(qcols + kcols, kcols)]),
        (wo, out_weight.at[shard]),
    ]
    weight_local = [
        pltpu.make_async_copy(src, dst, local_sem.at[3 + k]) for k, (src, dst) in enumerate(targets)
    ]

    barrier = pltpu.get_barrier_semaphore()
    greet = [{"hx": along_x}, {"hx": along_y}, {"hx": across}]
    greet += [{"hy": z_peers[j]} for j in (1, 2, 3)]
    if paired:
        greet.append({"tok": 1 - c})
    for peer in greet:
        pl.semaphore_signal(barrier, inc=1, device_id=peer, device_id_type=MESH)
    for copy in weight_local:
        copy.start()

    row8 = lax.broadcasted_iota(jnp.int32, (8, rows), 0)
    for copy in locals_[:3]:
        copy.wait()
    own = jnp.concatenate([slots[0, 0], slots[1, 0]], axis=1).astype(F32)

    def padded(vector):
        wide_vector = vector.astype(F32).reshape(1, width)
        return jnp.concatenate([wide_vector, jnp.zeros((1, rows + LANES - width), F32)], axis=1)

    before_row = padded(before_v[...])
    padded_tail = jnp.concatenate([before_row[:, rows:], jnp.zeros((1, rows - LANES), F32)], axis=1)
    head[...] = jnp.where(
        row8 == 0,
        jnp.sum(own * own, axis=0, keepdims=True),
        jnp.where(row8 == 1, before_row[:, :rows], jnp.where(row8 == 2, padded_tail, 0.0)),
    )
    pl.semaphore_wait(barrier, len(greet))

    def remote(src, dst, send, recv, peer):
        return pltpu.make_async_remote_copy(
            src_ref=src, dst_ref=dst, send_sem=send, recv_sem=recv, device_id=peer, device_id_type=MESH
        )

    def arrival(ref, sem):
        remote(ref, ref, sem, sem, {"hx": along_x}).wait_recv()

    def sent(ref, sem):
        remote(ref, ref, sem, sem, {"hx": along_x}).wait_send()

    def head_to_z(j):
        return remote(head, head_z.at[j - 1], send_sem.at[2], head_recv.at[0], {"hy": z_peers[j]})

    def head_to_plane(i):
        return remote(head_mid, head_plane.at[i - 1], send_sem.at[3], head_recv.at[1], {"hx": plane[i]})

    count = gather_recv.shape[1]
    part = width // count

    def gather(block, h, f):
        link = GATHER["AB"[h]][4 * block[0] + block[1]]
        origin = parent(block, link)
        k, rows_of = 4 * block[0] + block[1], pl.ds(f * part, part)
        return remote(
            slots.at[h, 4 * origin[0] + origin[1], rows_of], slots.at[h, k, rows_of],
            send_sem.at[0], gather_recv.at[h * 15 + k - 1, f], peers[link],
        )

    def piece_of(block, f):
        return pl.ds(pl.multiple_of(within(block[1]) + f * part, 16), part)

    def share(block, h, f):
        k = 4 * block[0] + block[1]
        link = REDUCE["AB"[h]][k]
        return remote(
            terms.at[h, block[0], piece_of(block, f)], shares.at[h, k, pl.ds(f * part, part)],
            send_sem.at[1], reduce_recv.at[h * 15 + k - 1, f], peers[link],
        )

    blocks = [(i, j) for i in range(4) for j in range(4)]
    children = {(h, block): [] for h in range(2) for block in blocks}
    for h in range(2):
        for block in blocks[1:]:
            link = REDUCE["AB"[h]][4 * block[0] + block[1]]
            children[h, parent(block, link)].append(block)

    weight_remote = []
    if paired:
        weight_remote = [
            remote(src, dst, send_sem.at[4], weight_recv.at[k], {"tok": 1 - c})
            for k, (src, dst) in enumerate(targets)
        ]
    state = {}
    arrived = set()

    def await_gather(block, h, f):
        if block != (0, 0) and ("g", block, h, f) not in arrived:
            arrived.add(("g", block, h, f))
            gather(block, h, f).wait_recv()

    def send_heads():
        for j in (3, 2, 1):
            head_to_z(j).start()

    def send_weights():
        for copy in weight_remote:
            copy.start()

    def relay_heads():
        arrival(head_z, head_recv.at[0])
        mains = [head[...]] + [head_z[j] for j in range(3)]
        total = mains[0] + mains[1] + mains[2] + mains[3]
        tails = jnp.zeros((1, rows), F32)
        for j in range(4):
            part = mains[j][2:3, :LANES]
            if j:
                part = pltpu.roll(tall_row(part), j * rest, 1)[0:1]
            tails = tails + jnp.concatenate([part, jnp.zeros((1, rows - LANES), F32)], axis=1)
        mid = jnp.where(row8 == 0, total[0:1], 0.0)
        for j in range(4):
            mid = jnp.where(row8 == 1 + j, mains[j][1:2], mid)
        head_mid[...] = jnp.where(row8 == 5, tails, mid)
        for i in (3, 1, 2):
            head_to_plane(i).start()

    def use_heads():
        arrival(head_plane, head_recv.at[1])
        groups = [head_mid[...]] + [head_plane[i] for i in range(3)]
        state["first_sq"] = groups[0][0:1] + groups[1][0:1] + groups[2][0:1] + groups[3][0:1]
        state["first_scale"] = lax.rsqrt(state["first_sq"] / D + epsilon)
        state["gain_columns"] = tall(jnp.concatenate(groups, axis=0))

    def turn_weights(first, amount):
        for k in range(amount // (4 * width)):
            at = pl.ds(pl.multiple_of(first + k * 4 * width, LANES), 4 * width)
            weights_t[:, at] = weights[at, :].T

    def own_weights():
        for copy in weight_local[:3]:
            copy.wait()
        turn_weights(start, wrows)

    def other_weights():
        for copy in weight_remote[:3]:
            copy.wait_recv()
        if paired:
            turn_weights(pl.multiple_of((1 - c) * wrows, LANES), wrows)

    def normalise(block, h):
        for f in range(count):
            await_gather(block, h, f)
        i, j = block
        gain_columns = state["gain_columns"]
        gain = jnp.concatenate(
            [gain_columns[:, 8 * i + 1 + j:8 * i + 2 + j], gain_columns[j * rest:(j + 1) * rest, 8 * i + 5:8 * i + 6]],
            axis=0,
        )
        scale = state["first_scale"][:, h * span:(h + 1) * span]
        normed[h, i, pl.ds(within(j), width), :] = (slots[h, 4 * i + j].astype(F32) * scale * gain).astype(BF16)

    def project(i, h):
        product = jnp.dot(weights_t[:, pl.ds(group(i), 4 * width)], normed[h, i], preferred_element_type=F32)
        if ("m", h) not in arrived:
            arrived.add(("m", h))
            acc[h] = product
        else:
            acc[h] += product

    shards, depth, columns = out_weight.shape

    def turn():
        weight_local[3].wait()
        for copy in weight_remote[3:]:
            copy.wait_recv()
        for copy in locals_[3:]:
            copy.wait()
        step = 3 * LANES
        for k in range(D // step):
            s, at = (k * step) // columns, (k * step) % columns
            out_t[k * step:(k + 1) * step, :] = out_weight[s, :, at:at + step].T
        doc_row = docs_v[...].astype(F32)
        after_row = padded(after_v[...])
        state["doc_row"] = doc_row
        state["doc_col"] = tall(jnp.broadcast_to(doc_row, (8, rows)))[:, 0:1]
        feed_row = padded(feed_v[...])
        state["feed"] = tall(jnp.broadcast_to(feed_row, (8, rows + LANES)))[:width, 0:1]
        state["after"] = tall(jnp.broadcast_to(after_row, (8, rows + LANES)))[:width, 0:1]

    query_heads, key_heads = qcols // HEAD, kcols // HEAD
    ratio = query_heads // key_heads

    def attend(h):
        lanes = slice(h * span, (h + 1) * span)
        seen = (h + 1) * span
        cosine, sine = tables_v[0, :, lanes], tables_v[1, :, lanes]

        def rope(x):
            upper, lower = x[:HEAD // 2], x[HEAD // 2:]
            return jnp.concatenate([upper * cosine - lower * sine, lower * cosine + upper * sine], axis=0)

        for kv in range(key_heads):
            keys[kv, :, lanes] = rope(acc[h, qcols + kv * HEAD:qcols + (kv + 1) * HEAD]).astype(BF16)
            values[kv, :, lanes] = acc[h, qcols + kcols + kv * HEAD:qcols + kcols + (kv + 1) * HEAD].astype(BF16)
        s_index = lax.broadcasted_iota(jnp.int32, (seen, span), 0)
        t_index = lax.broadcasted_iota(jnp.int32, (seen, span), 1) + h * span
        allowed = (s_index <= t_index) & (state["doc_row"][:, lanes] == state["doc_col"][:seen])
        for q in range(query_heads):
            query = (rope(acc[h, q * HEAD:(q + 1) * HEAD]) * (D / QH) ** (-0.5)).astype(BF16)
            key, value = keys[q // ratio, :, :seen], values[q // ratio, :, :seen]
            scores = lax.dot_general(key, query, (((0,), (0,)), ((), ())), preferred_element_type=F32)
            best = jnp.max(jnp.where(allowed, scores, neg_big), axis=0, keepdims=True)
            soft = jnp.where(allowed, jnp.exp(scores - best), 0.0)
            mass = jnp.sum(soft, axis=0, keepdims=True)
            blended = jnp.dot(value, soft.astype(BF16), preferred_element_type=F32)
            attended[h, q * HEAD:(q + 1) * HEAD, :] = (blended / mass).astype(BF16)

    def term(i, h):
        terms[h, i] = jnp.dot(
            out_t[pl.ds(group(i), 4 * width), :], attended[h], preferred_element_type=F32
        ).astype(BF16)

    def collect(block, h, f):
        for child in children[h, block]:
            share(child, h, f).wait_recv()
        total = terms[h, block[0], piece_of(block, f), :].astype(F32)
        for child in children[h, block]:
            total = total + shares[h, 4 * child[0] + child[1], f * part:(f + 1) * part].astype(F32)
        return total

    def pass_on(block, h, f):
        if children[h, block]:
            terms[h, block[0], piece_of(block, f), :] = collect(block, h, f).astype(BF16)
        share(block, h, f).start()

    def finish(h):
        lanes = slice(h * span, (h + 1) * span)
        sums = [0.0, 0.0, 0.0]
        for f in range(count):
            mixed = collect((0, 0), h, f)
            at = slice(f * part, (f + 1) * part)
            branch = mixed * state["after"][at]
            branch_v[at, lanes] = branch
            for k, product in enumerate((mixed * mixed, slots[h, 0, at].astype(F32) * branch, branch * branch)):
                sums[k] = sums[k] + jnp.sum(product, axis=0, keepdims=True)
        row4 = lax.broadcasted_iota(jnp.int32, (4, span), 0)
        stats[4 * h:4 * h + 4, :] = jnp.where(row4 == 0, sums[0], jnp.where(row4 == 1, sums[1], sums[2]))

    for task in ORDER:
        if task == "hz":
            send_heads()
        elif task == "hw":
            send_weights()
        elif task == "w0":
            own_weights()
        elif task == "w1":
            other_weights()
        elif task == "hm":
            relay_heads()
        elif task == "head":
            use_heads()
        elif task == "turn":
            turn()
        elif task[:3] == "fin":
            finish("AB".index(task[3]))
        elif task[0] == "a":
            attend("AB".index(task[1]))
        elif task[0] == "m":
            project(int(task[1]), "AB".index(task[2]))
        elif task[0] == "t":
            term(int(task[1]), "AB".index(task[2]))
        else:
            block, h = (int(task[1]), int(task[2])), "AB".index(task[3])
            f = int(task[4]) if len(task) > 4 else 0
            if task[0] == "s":
                await_gather(parent(block, GATHER["AB"[h]][4 * block[0] + block[1]]), h, f)
                gather(block, h, f).start()
            elif task[0] == "n":
                normalise(block, h)
            else:
                pass_on(block, h, f)

    def stat(i, j):
        k = 4 * i + j
        return remote(
            stats, stats_in.at[k - 1], send_sem.at[5], stat_recv.at[0], {"hx": flip(a, i), "hy": flip(b, j)}
        )

    far_first = sorted(blocks[1:], key=lambda block: -(bin(block[0]).count("1") + block[1]))
    for block in far_first:
        stat(*block).start()
    sent(shares.at[:, pl.ds(1, 15)], send_sem.at[0])
    sent(shares.at[:, pl.ds(1, 15)], send_sem.at[1])
    sent(head_z, send_sem.at[2])
    sent(head_plane, send_sem.at[3])
    if paired:
        sent(weights.at[pl.ds(0, wrows)], send_sem.at[4])
        sent(out_weight.at[0], send_sem.at[4])
    arrival(stats_in, stat_recv.at[0])
    packed = stats[...]
    for k in range(15):
        packed = packed + stats_in[k]
    summed = jnp.concatenate([packed[0:3], packed[4:7]], axis=1)
    after_scale = lax.rsqrt(summed[0:1] / D + epsilon)
    feed_sq = state["first_sq"] + 2.0 * after_scale * summed[1:2] + after_scale * after_scale * summed[2:3]
    feed_scale = lax.rsqrt(feed_sq / D + epsilon)
    for h in range(2):
        lanes = slice(h * span, (h + 1) * span)
        residual = (slots[h, 0].astype(F32) + branch_v[:, lanes] * after_scale[:, lanes]).astype(BF16)
        outs[0, :, lanes] = residual
        outs[1, :, lanes] = (residual.astype(F32) * feed_scale[:, lanes] * state["feed"]).astype(BF16)
    sent(stats_in, send_sem.at[5])


def per_device(paired, stream_in, before_gain, after_gain, feed_gain, query_weight, key_weight, value_weight, output_weight, documents):
    rows, width = stream_in.shape
    if not paired:
        query_weight, key_weight, value_weight = (
            lax.all_gather(piece, "tok", axis=0, tiled=True) for piece in (query_weight, key_weight, value_weight)
        )
        output_weight = lax.all_gather(output_weight, "tok", axis=1, tiled=True)
    tables = jnp.asarray(rope_tables())
    qcols, kcols = query_weight.shape[1], key_weight.shape[1]
    shards = 2 if paired else 1
    depth = output_weight.shape[0]
    any_spec = pl.BlockSpec(memory_space=pl.ANY)
    vmem = pl.BlockSpec(memory_space=pltpu.VMEM)
    dma = pltpu.SemaphoreType.DMA
    block, piece = (width, rows), (width, rows // 2)
    both = pl.pallas_call(
        functools.partial(kernel, paired),
        out_shape=pltpu.VMEM((2,) + block, BF16),
        in_specs=[any_spec] * 10,
        out_specs=vmem,
        scratch_shapes=[
            pltpu.VMEM((2, 16) + piece, BF16),
            pltpu.VMEM((1, rows), jnp.int32),
            pltpu.VMEM((width,), BF16),
            pltpu.VMEM((width,), BF16),
            pltpu.VMEM((width,), BF16),
            pltpu.VMEM(block, F32),
            pltpu.VMEM((2, HEAD // 2, LENGTH), F32),
            pltpu.VMEM((D, qcols + 2 * kcols), BF16),
            pltpu.VMEM((qcols + 2 * kcols, D), BF16),
            pltpu.VMEM((shards, depth, output_weight.shape[1]), BF16),
            pltpu.VMEM((D, depth), BF16),
            pltpu.VMEM((2, qcols + 2 * kcols, rows // 2), F32),
            pltpu.VMEM((kcols // HEAD, HEAD, rows), BF16),
            pltpu.VMEM((kcols // HEAD, HEAD, rows), BF16),
            pltpu.VMEM((2, qcols, rows // 2), BF16),
            pltpu.VMEM((2, 4, 4 * width, rows // 2), BF16),
            pltpu.VMEM((2, 4, 4 * width, rows // 2), BF16),
            pltpu.VMEM((2, 16) + piece, BF16),
        ]
        + [pltpu.VMEM((8, rows), F32), pltpu.VMEM((3, 8, rows), F32)] * 2
        + [pltpu.VMEM((8, rows // 2), F32), pltpu.VMEM((15, 8, rows // 2), F32)]
        + [
            dma((11,)),
            dma((6,)),
            dma((4,)),
            dma((30, PIECES)),
            dma((30, PIECES)),
            dma((2,)),
            dma((1,)),
        ],
        compiler_params=pltpu.CompilerParams(
            collective_id=0, has_side_effects=True, vmem_limit_bytes=56 * 1024 * 1024
        ),
    )(
        stream_in.T,
        documents.reshape(1, rows),
        before_gain,
        after_gain,
        feed_gain,
        tables,
        query_weight,
        key_weight,
        value_weight,
        output_weight,
    )
    return both[0].T, both[1].T


def solution(mesh):
    both = ("hx", "hy")
    in_specs = (
        P("tok", both),
        P(both),
        P(both),
        P(both),
        P("tok", both),
        P("tok", both),
        P("tok", both),
        P(both, "tok"),
        P("tok"),
    )
    out_specs = (P("tok", both), P("tok", both))
    paired = mesh.shape["tok"] == 2
    return jax.shard_map(
        functools.partial(per_device, paired), mesh=mesh, in_specs=in_specs, out_specs=out_specs, check_vma=False
    )
```

```python
import functools

import jax
import jax.numpy as jnp
import numpy as np
from jax import lax
from jax.experimental import pallas as pl
from jax.experimental.pallas import tpu as pltpu
from jax.sharding import PartitionSpec as P

D = 4608
QH = 32
HEAD = 128
LENGTH = 256
LANES = 128

epsilon = 1e-06
neg_big = -1e30
MESH = pl.DeviceIdType.MESH
F32 = jnp.float32
BF16 = jnp.bfloat16


GATHER_0 = (
    (-1, 3, 4, 3, 0, 0, 0, 3, 1, 1, 1, 1, 2, 0, 0, 1),
    (-1, 3, 4, 3, 0, 3, 0, 3, 1, 3, 1, 3, 2, 0, 1, 2),
)
REDUCE_0 = (
    (-1, 3, 4, 5, 0, 3, 0, 0, 1, 3, 1, 1, 0, 1, 3, 2),
    (-1, 3, 4, 3, 0, 0, 0, 0, 1, 1, 1, 1, 2, 3, 2, 3),
)
ORDER_0 = (
    2, 20, 8, 116, 117, 1, 18, 4, 28, 12, 24, 3, 6, 10, 120, 118, 25, 5, 9, 7,
    22, 19, 11, 14, 119, 121, 32, 21, 60, 52, 34, 26, 37, 122, 13, 40, 38, 15, 17, 41,
    43, 33, 35, 39, 30, 96, 29, 36, 51, 46, 27, 31, 54, 42, 58, 97, 98, 50, 23, 45,
    53, 57, 48, 56, 44, 47, 99, 112, 107, 78, 77, 76, 106, 74, 62, 105, 104, 61, 59, 65,
    70, 102, 49, 100, 75, 71, 73, 63, 55, 103, 101, 113, 111, 95, 79, 69, 93, 66, 109, 110,
    87, 86, 91, 90, 94, 108, 85, 83, 67, 68, 84, 89, 72, 82, 88, 92, 81, 114, 115,
)
GATHER_1 = (
    (-1, 3, 3, 5, 0, 0, 0, 0, 1, 1, 3, 1, 0, 1, 3, 1),
    (-1, 3, 3, 5, 0, 0, 0, 0, 1, 3, 3, 1, 1, 2, 2, 1),
)
REDUCE_1 = (
    (-1, 3, 4, 5, 0, 0, 3, 0, 1, 1, 1, 1, 0, 3, 0, 1),
    (-1, 3, 3, 5, 0, 3, 0, 0, 1, 1, 3, 1, 2, 0, 3, 1),
)
ORDER_1 = (
    8, 20, 116, 117, 17, 24, 4, 3, 12, 1, 19, 28, 118, 29, 7, 5, 2, 11, 119, 9,
    44, 32, 25, 40, 21, 56, 120, 121, 18, 35, 52, 33, 23, 15, 27, 61, 122, 43, 10, 6,
    60, 39, 13, 36, 37, 49, 41, 34, 96, 57, 48, 50, 51, 14, 53, 100, 30, 22, 55, 47,
    26, 42, 59, 98, 31, 38, 97, 45, 46, 99, 112, 105, 106, 73, 70, 69, 62, 107, 58, 102,
    77, 79, 78, 75, 54, 63, 101, 103, 113, 111, 93, 94, 109, 86, 85, 74, 104, 108, 71, 110,
    76, 90, 95, 65, 66, 89, 82, 91, 87, 72, 68, 67, 84, 88, 92, 83, 81, 114, 115,
)
PLANS = ((GATHER_0, REDUCE_0, ORDER_0), (GATHER_1, REDUCE_1, ORDER_1))


def flip(index, mask):
    low = (index % 2 + mask % 2) % 2
    high = (index // 2 + mask // 2) % 2
    return low + 2 * high


def rope_tables():
    half = HEAD // 2
    frequency = (10000.0 ** (-np.arange(half, dtype=np.float32) / half)).astype(np.float32)
    angles = frequency[:, None] * np.arange(LENGTH, dtype=np.float32)[None, :]
    return np.stack([np.cos(angles), np.sin(angles)]).astype(np.float32)


def tall_row(row):
    return jnp.broadcast_to(row, (8, row.shape[1]))


def tall(block):
    return jnp.concatenate([block] * (LANES // block.shape[0]), axis=0).T


def parent(block, link):
    i, j = block
    return (i ^ (link + 1), j) if link < 3 else (i, j ^ (link - 2))


def kernel(
    paired,
    stream, docs, before, after_in, feed_in, tables, wq, wk, wv, wo,
    outs,
    slots, docs_v, before_v, after_v, feed_v, branch_v, tables_v, weights, weights_t, out_weight, out_t, acc, keys, values, attended,
    normed, terms, shares, head, head_z, head_mid, head_plane, stats, stats_in,
    local_sem, send_sem, weight_recv, gather_recv, reduce_recv, head_recv, stat_recv,
):
    width, rows = stream.shape
    rest = width - rows
    span = rows // 2
    a, b, c = lax.axis_index("hx"), lax.axis_index("hy"), lax.axis_index("tok")
    along_x, along_y, across = flip(a, 1), flip(a, 2), flip(a, 3)
    plane = (None, along_x, along_y, across)
    z_peers = [None] + [flip(b, j) for j in (1, 2, 3)]
    peers = [{"hx": along_x}, {"hx": along_y}, {"hx": across}] + [{"hy": z_peers[j]} for j in (1, 2, 3)]

    def group(i):
        return pl.multiple_of(flip(a, i) * (4 * width), LANES)

    def within(j):
        return pl.multiple_of(flip(b, j) * width, 16)

    locals_ = [
        pltpu.make_async_copy(stream.at[:, pl.ds(0, span)], slots.at[0, 0], local_sem.at[0]),
        pltpu.make_async_copy(stream.at[:, pl.ds(span, span)], slots.at[1, 0], local_sem.at[9]),
        pltpu.make_async_copy(before, before_v, local_sem.at[1]),
        pltpu.make_async_copy(tables, tables_v, local_sem.at[2]),
        pltpu.make_async_copy(docs, docs_v, local_sem.at[7]),
        pltpu.make_async_copy(after_in, after_v, local_sem.at[8]),
        pltpu.make_async_copy(feed_in, feed_v, local_sem.at[10]),
    ]
    for copy in locals_:
        copy.start()
    wrows, qcols, kcols = wq.shape[0], wq.shape[1], wk.shape[1]
    shard = c if paired else 0
    start = pl.multiple_of(shard * wrows, LANES)
    targets = [
        (wq, weights.at[pl.ds(start, wrows), pl.ds(0, qcols)]),
        (wk, weights.at[pl.ds(start, wrows), pl.ds(qcols, kcols)]),
        (wv, weights.at[pl.ds(start, wrows), pl.ds(qcols + kcols, kcols)]),
        (wo, out_weight.at[shard]),
    ]
    weight_local = [
        pltpu.make_async_copy(src, dst, local_sem.at[3 + k]) for k, (src, dst) in enumerate(targets)
    ]

    barrier = pltpu.get_barrier_semaphore()
    greet = [{"hx": along_x}, {"hx": along_y}, {"hx": across}]
    greet += [{"hy": z_peers[j]} for j in (1, 2, 3)]
    if paired:
        greet.append({"tok": 1 - c})
    for peer in greet:
        pl.semaphore_signal(barrier, inc=1, device_id=peer, device_id_type=MESH)
    for copy in weight_local:
        copy.start()

    row8 = lax.broadcasted_iota(jnp.int32, (8, rows), 0)
    for copy in locals_[:3]:
        copy.wait()
    own = jnp.concatenate([slots[0, 0], slots[1, 0]], axis=1).astype(F32)

    def padded(vector):
        wide_vector = vector.astype(F32).reshape(1, width)
        return jnp.concatenate([wide_vector, jnp.zeros((1, rows + LANES - width), F32)], axis=1)

    before_row = padded(before_v[...])
    padded_tail = jnp.concatenate([before_row[:, rows:], jnp.zeros((1, rows - LANES), F32)], axis=1)
    head[...] = jnp.where(
        row8 == 0,
        jnp.sum(own * own, axis=0, keepdims=True),
        jnp.where(row8 == 1, before_row[:, :rows], jnp.where(row8 == 2, padded_tail, 0.0)),
    )
    pl.semaphore_wait(barrier, len(greet))

    def run(gather_links, reduce_links, order):

        def remote(src, dst, send, recv, peer):
            return pltpu.make_async_remote_copy(
                src_ref=src, dst_ref=dst, send_sem=send, recv_sem=recv, device_id=peer, device_id_type=MESH
            )

        def arrival(ref, sem):
            remote(ref, ref, sem, sem, {"hx": along_x}).wait_recv()

        def sent(ref, sem):
            remote(ref, ref, sem, sem, {"hx": along_x}).wait_send()

        def head_to_z(j):
            return remote(head, head_z.at[j - 1], send_sem.at[2], head_recv.at[0], {"hy": z_peers[j]})

        def head_to_plane(i):
            return remote(head_mid, head_plane.at[i - 1], send_sem.at[3], head_recv.at[1], {"hx": plane[i]})

        count = gather_recv.shape[1]
        part = width // count

        def gather(block, h, f):
            link = gather_links[h][4 * block[0] + block[1]]
            origin = parent(block, link)
            k, rows_of = 4 * block[0] + block[1], pl.ds(f * part, part)
            return remote(
                slots.at[h, 4 * origin[0] + origin[1], rows_of], slots.at[h, k, rows_of],
                send_sem.at[0], gather_recv.at[h * 15 + k - 1, f], peers[link],
            )

        def piece_of(block, f):
            return pl.ds(pl.multiple_of(within(block[1]) + f * part, 16), part)

        def share(block, h, f):
            k = 4 * block[0] + block[1]
            link = reduce_links[h][k]
            return remote(
                terms.at[h, block[0], piece_of(block, f)], shares.at[h, k, pl.ds(f * part, part)],
                send_sem.at[1], reduce_recv.at[h * 15 + k - 1, f], peers[link],
            )

        blocks = [(i, j) for i in range(4) for j in range(4)]
        children = {(h, block): [] for h in range(2) for block in blocks}
        for h in range(2):
            for block in blocks[1:]:
                link = reduce_links[h][4 * block[0] + block[1]]
                children[h, parent(block, link)].append(block)

        weight_remote = []
        if paired:
            weight_remote = [
                remote(src, dst, send_sem.at[4], weight_recv.at[k], {"tok": 1 - c})
                for k, (src, dst) in enumerate(targets)
            ]
        state = {}
        arrived = set()

        def await_gather(block, h, f):
            if block != (0, 0) and ("g", block, h, f) not in arrived:
                arrived.add(("g", block, h, f))
                gather(block, h, f).wait_recv()

        def send_heads():
            for j in (3, 2, 1):
                head_to_z(j).start()

        def send_weights():
            for copy in weight_remote:
                copy.start()

        def relay_heads():
            arrival(head_z, head_recv.at[0])
            mains = [head[...]] + [head_z[j] for j in range(3)]
            total = mains[0] + mains[1] + mains[2] + mains[3]
            tails = jnp.zeros((1, rows), F32)
            for j in range(4):
                part = mains[j][2:3, :LANES]
                if j:
                    part = pltpu.roll(tall_row(part), j * rest, 1)[0:1]
                tails = tails + jnp.concatenate([part, jnp.zeros((1, rows - LANES), F32)], axis=1)
            mid = jnp.where(row8 == 0, total[0:1], 0.0)
            for j in range(4):
                mid = jnp.where(row8 == 1 + j, mains[j][1:2], mid)
            head_mid[...] = jnp.where(row8 == 5, tails, mid)
            for i in (3, 1, 2):
                head_to_plane(i).start()

        def use_heads():
            arrival(head_plane, head_recv.at[1])
            groups = [head_mid[...]] + [head_plane[i] for i in range(3)]
            state["first_sq"] = groups[0][0:1] + groups[1][0:1] + groups[2][0:1] + groups[3][0:1]
            state["first_scale"] = lax.rsqrt(state["first_sq"] / D + epsilon)
            state["gain_columns"] = tall(jnp.concatenate(groups, axis=0))

        def turn_weights(first, amount):
            for k in range(amount // (4 * width)):
                at = pl.ds(pl.multiple_of(first + k * 4 * width, LANES), 4 * width)
                weights_t[:, at] = weights[at, :].T

        def own_weights():
            for copy in weight_local[:3]:
                copy.wait()
            turn_weights(start, wrows)

        def other_weights():
            for copy in weight_remote[:3]:
                copy.wait_recv()
            if paired:
                turn_weights(pl.multiple_of((1 - c) * wrows, LANES), wrows)

        def normalise(block, h):
            for f in range(count):
                await_gather(block, h, f)
            i, j = block
            gain_columns = state["gain_columns"]
            gain = jnp.concatenate(
                [gain_columns[:, 8 * i + 1 + j:8 * i + 2 + j], gain_columns[j * rest:(j + 1) * rest, 8 * i + 5:8 * i + 6]],
                axis=0,
            )
            scale = state["first_scale"][:, h * span:(h + 1) * span]
            normed[h, i, pl.ds(within(j), width), :] = (slots[h, 4 * i + j].astype(F32) * scale * gain).astype(BF16)

        def project(i, h):
            product = jnp.dot(weights_t[:, pl.ds(group(i), 4 * width)], normed[h, i], preferred_element_type=F32)
            if ("m", h) not in arrived:
                arrived.add(("m", h))
                acc[h] = product
            else:
                acc[h] += product

        shards, depth, columns = out_weight.shape

        def turn():
            weight_local[3].wait()
            for copy in weight_remote[3:]:
                copy.wait_recv()
            for copy in locals_[3:]:
                copy.wait()
            step = 3 * LANES
            for k in range(D // step):
                s, at = (k * step) // columns, (k * step) % columns
                out_t[k * step:(k + 1) * step, :] = out_weight[s, :, at:at + step].T
            doc_row = docs_v[...].astype(F32)
            after_row = padded(after_v[...])
            state["doc_row"] = doc_row
            state["doc_col"] = tall(jnp.broadcast_to(doc_row, (8, rows)))[:, 0:1]
            feed_row = padded(feed_v[...])
            state["feed"] = tall(jnp.broadcast_to(feed_row, (8, rows + LANES)))[:width, 0:1]
            state["after"] = tall(jnp.broadcast_to(after_row, (8, rows + LANES)))[:width, 0:1]

        query_heads, key_heads = qcols // HEAD, kcols // HEAD
        ratio = query_heads // key_heads

        def attend(h):
            lanes = slice(h * span, (h + 1) * span)
            seen = (h + 1) * span
            cosine, sine = tables_v[0, :, lanes], tables_v[1, :, lanes]

            def rope(x):
                upper, lower = x[:HEAD // 2], x[HEAD // 2:]
                return jnp.concatenate([upper * cosine - lower * sine, lower * cosine + upper * sine], axis=0)

            for kv in range(key_heads):
                keys[kv, :, lanes] = rope(acc[h, qcols + kv * HEAD:qcols + (kv + 1) * HEAD]).astype(BF16)
                values[kv, :, lanes] = acc[h, qcols + kcols + kv * HEAD:qcols + kcols + (kv + 1) * HEAD].astype(BF16)
            s_index = lax.broadcasted_iota(jnp.int32, (seen, span), 0)
            t_index = lax.broadcasted_iota(jnp.int32, (seen, span), 1) + h * span
            allowed = (s_index <= t_index) & (state["doc_row"][:, lanes] == state["doc_col"][:seen])
            for q in range(query_heads):
                query = (rope(acc[h, q * HEAD:(q + 1) * HEAD]) * (D / QH) ** (-0.5)).astype(BF16)
                key, value = keys[q // ratio, :, :seen], values[q // ratio, :, :seen]
                scores = lax.dot_general(key, query, (((0,), (0,)), ((), ())), preferred_element_type=F32)
                best = jnp.max(jnp.where(allowed, scores, neg_big), axis=0, keepdims=True)
                soft = jnp.where(allowed, jnp.exp(scores - best), 0.0)
                mass = jnp.sum(soft, axis=0, keepdims=True)
                blended = jnp.dot(value, soft.astype(BF16), preferred_element_type=F32)
                attended[h, q * HEAD:(q + 1) * HEAD, :] = (blended / mass).astype(BF16)

        def term(i, h):
            terms[h, i] = jnp.dot(
                out_t[pl.ds(group(i), 4 * width), :], attended[h], preferred_element_type=F32
            ).astype(BF16)

        def collect(block, h, f):
            for child in children[h, block]:
                share(child, h, f).wait_recv()
            total = terms[h, block[0], piece_of(block, f), :].astype(F32)
            for child in children[h, block]:
                total = total + shares[h, 4 * child[0] + child[1], f * part:(f + 1) * part].astype(F32)
            return total

        def pass_on(block, h, f):
            if children[h, block]:
                terms[h, block[0], piece_of(block, f), :] = collect(block, h, f).astype(BF16)
            share(block, h, f).start()

        def finish(h):
            lanes = slice(h * span, (h + 1) * span)
            sums = [0.0, 0.0, 0.0]
            for f in range(count):
                mixed = collect((0, 0), h, f)
                at = slice(f * part, (f + 1) * part)
                branch = mixed * state["after"][at]
                branch_v[at, lanes] = branch
                for k, product in enumerate((mixed * mixed, slots[h, 0, at].astype(F32) * branch, branch * branch)):
                    sums[k] = sums[k] + jnp.sum(product, axis=0, keepdims=True)
            row4 = lax.broadcasted_iota(jnp.int32, (4, span), 0)
            stats[4 * h:4 * h + 4, :] = jnp.where(row4 == 0, sums[0], jnp.where(row4 == 1, sums[1], sums[2]))

        singles = (send_heads, send_weights, relay_heads, use_heads, own_weights, other_weights, turn)
        for task in order:
            h, k = task % 32 // 16, task % 16
            block = (k // 4, k % 4)
            if task < 32:
                await_gather(parent(block, gather_links[h][k]), h, 0)
                gather(block, h, 0).start()
            elif task < 64:
                normalise(block, h)
            elif task < 96:
                pass_on(block, h, 0)
            elif task < 104:
                project(task % 4, (task - 96) // 4)
            elif task < 112:
                term(task % 4, (task - 104) // 4)
            elif task < 114:
                attend(task - 112)
            elif task < 116:
                finish(task - 114)
            else:
                singles[task - 116]()

        def stat(i, j):
            k = 4 * i + j
            return remote(
                stats, stats_in.at[k - 1], send_sem.at[5], stat_recv.at[0], {"hx": flip(a, i), "hy": flip(b, j)}
            )

        far_first = sorted(blocks[1:], key=lambda block: -(bin(block[0]).count("1") + block[1]))
        for block in far_first:
            stat(*block).start()
        sent(shares.at[:, pl.ds(1, 15)], send_sem.at[0])
        sent(shares.at[:, pl.ds(1, 15)], send_sem.at[1])
        sent(head_z, send_sem.at[2])
        sent(head_plane, send_sem.at[3])
        if paired:
            sent(weights.at[pl.ds(0, wrows)], send_sem.at[4])
            sent(out_weight.at[0], send_sem.at[4])
        arrival(stats_in, stat_recv.at[0])
        packed = stats[...]
        for k in range(15):
            packed = packed + stats_in[k]
        summed = jnp.concatenate([packed[0:3], packed[4:7]], axis=1)
        after_scale = lax.rsqrt(summed[0:1] / D + epsilon)
        feed_sq = state["first_sq"] + 2.0 * after_scale * summed[1:2] + after_scale * after_scale * summed[2:3]
        feed_scale = lax.rsqrt(feed_sq / D + epsilon)
        for h in range(2):
            lanes = slice(h * span, (h + 1) * span)
            residual = (slots[h, 0].astype(F32) + branch_v[:, lanes] * after_scale[:, lanes]).astype(BF16)
            outs[0, :, lanes] = residual
            outs[1, :, lanes] = (residual.astype(F32) * feed_scale[:, lanes] * state["feed"]).astype(BF16)
        sent(stats_in, send_sem.at[5])

    for core in range(2):
        pl.when(c % 2 == core)(functools.partial(run, *PLANS[core]))


def per_device(paired, stream_in, before_gain, after_gain, feed_gain, query_weight, key_weight, value_weight, output_weight, documents):
    rows, width = stream_in.shape
    if not paired:
        query_weight, key_weight, value_weight = (
            lax.all_gather(piece, "tok", axis=0, tiled=True) for piece in (query_weight, key_weight, value_weight)
        )
        output_weight = lax.all_gather(output_weight, "tok", axis=1, tiled=True)
    tables = jnp.asarray(rope_tables())
    qcols, kcols = query_weight.shape[1], key_weight.shape[1]
    shards = 2 if paired else 1
    depth = output_weight.shape[0]
    any_spec = pl.BlockSpec(memory_space=pl.ANY)
    vmem = pl.BlockSpec(memory_space=pltpu.VMEM)
    dma = pltpu.SemaphoreType.DMA
    block, piece = (width, rows), (width, rows // 2)
    both = pl.pallas_call(
        functools.partial(kernel, paired),
        out_shape=pltpu.VMEM((2,) + block, BF16),
        in_specs=[any_spec] * 10,
        out_specs=vmem,
        scratch_shapes=[
            pltpu.VMEM((2, 16) + piece, BF16),
            pltpu.VMEM((1, rows), jnp.int32),
            pltpu.VMEM((width,), BF16),
            pltpu.VMEM((width,), BF16),
            pltpu.VMEM((width,), BF16),
            pltpu.VMEM(block, F32),
            pltpu.VMEM((2, HEAD // 2, LENGTH), F32),
            pltpu.VMEM((D, qcols + 2 * kcols), BF16),
            pltpu.VMEM((qcols + 2 * kcols, D), BF16),
            pltpu.VMEM((shards, depth, output_weight.shape[1]), BF16),
            pltpu.VMEM((D, depth), BF16),
            pltpu.VMEM((2, qcols + 2 * kcols, rows // 2), F32),
            pltpu.VMEM((kcols // HEAD, HEAD, rows), BF16),
            pltpu.VMEM((kcols // HEAD, HEAD, rows), BF16),
            pltpu.VMEM((2, qcols, rows // 2), BF16),
            pltpu.VMEM((2, 4, 4 * width, rows // 2), BF16),
            pltpu.VMEM((2, 4, 4 * width, rows // 2), BF16),
            pltpu.VMEM((2, 16) + piece, BF16),
        ]
        + [pltpu.VMEM((8, rows), F32), pltpu.VMEM((3, 8, rows), F32)] * 2
        + [pltpu.VMEM((8, rows // 2), F32), pltpu.VMEM((15, 8, rows // 2), F32)]
        + [
            dma((11,)),
            dma((6,)),
            dma((4,)),
            dma((30, 1)),
            dma((30, 1)),
            dma((2,)),
            dma((1,)),
        ],
        compiler_params=pltpu.CompilerParams(
            collective_id=0, has_side_effects=True, vmem_limit_bytes=56 * 1024 * 1024
        ),
    )(
        stream_in.T,
        documents.reshape(1, rows),
        before_gain,
        after_gain,
        feed_gain,
        tables,
        query_weight,
        key_weight,
        value_weight,
        output_weight,
    )
    return both[0].T, both[1].T


def solution(mesh):
    both = ("hx", "hy")
    in_specs = (
        P("tok", both),
        P(both),
        P(both),
        P(both),
        P("tok", both),
        P("tok", both),
        P("tok", both),
        P(both, "tok"),
        P("tok"),
    )
    out_specs = (P("tok", both), P("tok", both))
    paired = mesh.shape["tok"] == 2
    return jax.shard_map(
        functools.partial(per_device, paired), mesh=mesh, in_specs=in_specs, out_specs=out_specs, check_vma=False
    )
```
